32 devices in a mesh: dom: 16 (over z, y, x), feat: 2 (over core).
Axes of the slice: x: 2, y: 2, z: 4, core: 2. Of those that a mesh axis runs over, the one named last changes fastest.
Arguments:
- features: bfloat16 [32768, 608], P('dom', 'feat'), may hold values from -6 to 6
- weight: bfloat16 [608, 256], replicated, may hold values from -0.25 to 0.25
- out_bias: float32 [256], P('feat'), may hold values from -3 to 3
- tile_values: bfloat16 [1728, 128, 128], P('dom'), may hold values from -0.25 to 0.25
- tile_rows: int32 [1728], P('dom'), may hold values from 0 to 15
- tile_cols: int32 [1728], P('dom'), may hold values from 0 to 81, as said below
- tile_count: int32 [16], P('dom'), may hold values from 10 to 108, as said below
- send_rows: int32 [16, 8, 1024], P('dom'), may hold values from 0 to 2047
- hub_ids: int32 [256], replicated, may hold values from 0 to 32767, as said below
Outputs:
- activations: bfloat16 [32768, 256], P('dom', 'feat')
The draws below stay inside these ranges and needn't reach their ends.
Inputs may be any that keep to these rules, and one draw needn't show every extreme that they name: `tile_count`: slots at or past a partition's count are not part of the graph; some partition uses all 108 slots. `tile_cols`: column blocks index the extended row space of the slot's partition. `hub_ids`: distinct vertex ids; vertex v belongs to partition v // 2048; no partition owns more than 48 hubs, and some partition owns exactly 48.
All inputs are finite; a program needn't handle non-finite values.
Results may differ from the reference program's by a relative error of at most 0.0044.
Values may be sent and summed in bfloat16 or wider, within the bound.
A program may use at most 64 MiB of HBM per device.

```python
import jax
import jax.numpy as jnp
from jax import lax

F_IN = 608
HID = 256
BLK = 128
VDEV = 2048
REACH = 4
HUB_MOST = 48
TILE_MOST = 108
HALO = 1024
HUBS = 256
EXT = 10496
VERTICES = 32768
PARTITIONS = 16
TILES = 1728
N_DOM = 16


def draw_tile_count(key, part):
    lowest = 2 * REACH + 2
    spread = TILE_MOST - lowest + 1
    key_list = jax.random.split(jax.random.fold_in(key, 11), 2)
    raw_draws = jax.random.randint(key_list[0], (N_DOM,), 0, spread)
    counts = lowest + raw_draws * raw_draws // spread
    fullest = jax.random.randint(key_list[1], (), 0, N_DOM)
    counts = jnp.where(jnp.arange(N_DOM) == fullest, TILE_MOST, counts)
    return counts.astype(jnp.int32)


def draw_tile_cols(key, part):
    block_total = ((1 + REACH) * VDEV + HUBS) // BLK
    hub_first = (1 + REACH) * VDEV // BLK
    key_list = jax.random.split(jax.random.fold_in(key, 23), 3)
    columns = jax.random.randint(key_list[0], (N_DOM, TILE_MOST), 0, block_total)
    position = jnp.arange(TILE_MOST)[None, :]
    segment_start = (VDEV + position * (VDEV // 2)) // BLK
    hub_pick = jax.random.randint(key_list[1], (N_DOM, 1), hub_first, block_total)
    local_pick = jax.random.randint(key_list[2], (N_DOM, 1), 0, VDEV // BLK)
    columns = jnp.where(position < 2 * REACH, segment_start, columns)
    columns = jnp.where(position == 2 * REACH, hub_pick, columns)
    columns = jnp.where(position == 2 * REACH + 1, local_pick, columns)
    return columns.reshape(N_DOM * TILE_MOST).astype(jnp.int32)


def draw_hub_ids(key, part):
    key_list = jax.random.split(jax.random.fold_in(key, 37), 4)
    slot_total = N_DOM * HUB_MOST
    positions = jnp.arange(slot_total)
    owners = positions // HUB_MOST
    ranks = positions % HUB_MOST
    device_level = jax.random.randint(key_list[0], (N_DOM,), 0, 4)
    fullest = jax.random.randint(key_list[1], (), 0, N_DOM)
    jitter = jax.random.randint(key_list[2], (slot_total,), 0, 1024)
    scores = (device_level[owners] * 1024 + jitter) * slot_total + positions
    scores = jnp.where(owners == fullest, scores + 8 * 1024 * slot_total, scores)
    chosen = jax.lax.top_k(scores.astype(jnp.int32), HUBS)[1]
    stride = VDEV // HUB_MOST
    shifts = jax.random.randint(key_list[3], (N_DOM,), 0, stride)
    chosen_owner = owners[chosen]
    local_rows = ranks[chosen] * stride + shifts[chosen_owner]
    return (chosen_owner * VDEV + local_rows).astype(jnp.int32)


def with_ends(drawn, own_key, smallest, largest):
    longest = drawn.shape.index(max(drawn.shape))
    spots = []
    for shift in (0, 1):
        where = [jax.random.randint(jax.random.fold_in(own_key, axis), (), 0, length) for axis, length in enumerate(drawn.shape)]
        where[longest] = (where[longest] + shift) % drawn.shape[longest]
        spots.append(tuple(where))
    return drawn.at[spots[0]].set(smallest).at[spots[1]].set(largest)


def block_levels(own_key, shape, cuts, low, top_value):
    level, own = 1.0, jax.random.fold_in(own_key, 6)
    for dim, blocks in cuts:
        draws = jnp.exp(jax.random.uniform(jax.random.fold_in(own, dim), (blocks,), jnp.float32, low / len(cuts), top_value / len(cuts)))
        level = level * jnp.repeat(draws, shape[dim] // blocks).reshape([-1 if axis == dim else 1 for axis in range(len(shape))])
    return level


def bell_draw(rng, extent, scale, bound, cuts=(), kind=jnp.bfloat16):
    values = jax.random.normal(rng, extent, jnp.float32) * scale
    if len(cuts) > 0:
        values = block_levels(rng, extent, cuts, -0.22, 0.18) * values
    return jnp.clip(values, min=-bound, max=bound).astype(kind)


def setup_inputs(seed: int = 0) -> dict:
    seeds = jax.random.split(jax.random.key(seed), 10)
    features = bell_draw(seeds[0], (VERTICES, F_IN), 1.0, 6.0, ((0, 16), (1, 2)))
    weight = bell_draw(seeds[1], (F_IN, HID), F_IN ** -0.5, 0.25)
    out_bias = bell_draw(seeds[2], (HID,), 0.5, 3.0, ((0, 2),), jnp.float32)
    tile_values = bell_draw(seeds[3], (TILES, BLK, BLK), (4 * BLK) ** -0.5, 0.25, ((0, 16),))
    tile_rows = with_ends(jax.random.randint(seeds[4], (TILES,), 0, VDEV // BLK), jax.random.fold_in(seeds[4], 1), 0, (VDEV // BLK) - 1).astype(jnp.int32)
    tile_cols = draw_tile_cols(jax.random.fold_in(seeds[9], 71), 0)
    tile_count = draw_tile_count(jax.random.fold_in(seeds[9], 71), 0)
    send_rows = with_ends(jax.random.randint(seeds[7], (PARTITIONS, 2 * REACH, HALO), 0, VDEV), jax.random.fold_in(seeds[7], 1), 0, VDEV - 1).astype(jnp.int32)
    hub_ids = draw_hub_ids(jax.random.fold_in(seeds[9], 71), 0)
    return {"features": features, "weight": weight, "out_bias": out_bias, "tile_values": tile_values, "tile_rows": tile_rows, "tile_cols": tile_cols, "tile_count": tile_count, "send_rows": send_rows, "hub_ids": hub_ids}


def reference(features, weight, out_bias, tile_values, tile_rows, tile_cols, tile_count, send_rows, hub_ids):
    projected = jnp.dot(features, weight, preferred_element_type=jnp.float32).astype(jnp.bfloat16)
    hub_rows = projected[hub_ids]
    offsets = jnp.array(list(range(-REACH, 0)) + list(range(1, REACH + 1)), jnp.int32)
    slot_ids = jnp.arange(2 * REACH).astype(jnp.int32)

    def one_partition(partition):
        own_rows = lax.dynamic_slice_in_dim(projected, partition * VDEV, VDEV, 0)
        sources = partition - offsets
        present = (sources >= 0) & (sources < N_DOM)
        clipped = jnp.clip(sources, 0, N_DOM - 1).astype(jnp.int32)
        listed = send_rows[clipped, slot_ids]
        picked = projected[clipped[:, None] * VDEV + listed]
        picked = jnp.where(present[:, None, None], picked, jnp.zeros_like(picked))
        extended = jnp.concatenate([own_rows, picked.reshape(REACH * VDEV, HID), hub_rows], 0)
        blocks = extended.reshape(EXT // BLK, BLK, HID)
        col_blocks = lax.dynamic_slice_in_dim(tile_cols, partition * TILE_MOST, TILE_MOST, 0)
        row_blocks = lax.dynamic_slice_in_dim(tile_rows, partition * TILE_MOST, TILE_MOST, 0)
        own_tiles = lax.dynamic_slice_in_dim(tile_values, partition * TILE_MOST, TILE_MOST, 0)
        products = jnp.einsum("tij,tjc->tic", own_tiles.astype(jnp.float32), blocks[col_blocks].astype(jnp.float32), precision=lax.Precision.HIGHEST)
        live_mask = jnp.arange(TILE_MOST).astype(jnp.int32) < tile_count[partition]
        products = jnp.where(live_mask[:, None, None], products, jnp.zeros_like(products))
        aggregate = jax.ops.segment_sum(products, row_blocks, num_segments=VDEV // BLK)
        return jnp.maximum(aggregate.reshape(VDEV, HID) + out_bias, 0.0).astype(jnp.bfloat16)

    result = lax.map(one_partition, jnp.arange(N_DOM, dtype=jnp.int32))
    return result.reshape(N_DOM * VDEV, HID)
```

```python
import functools
import math

import jax
import jax.numpy as jnp
from jax import lax
from jax.experimental import pallas as pl
from jax.experimental.pallas import tpu as pltpu
from jax.sharding import PartitionSpec as P

REACH = 4
HUB_MOST = 48


def passed_along(value, axis, steps):
    count = lax.axis_size(axis)
    initial, last = (max(0, -steps), min(count, count - steps))
    return lax.ppermute(value, axis, [(source, source + steps) for source in range(initial, last)])


def local_any(
    features, weight, out_bias, tile_values, tile_rows, tile_cols, tile_count, send_rows, hub_ids
):
    column_count = out_bias.shape[0]
    vertex_rows = features.shape[0]
    part_index = lax.axis_index("dom")
    feat_index = lax.axis_index("feat")
    weight_cols = lax.dynamic_slice_in_dim(weight, feat_index * column_count, column_count, 1)
    summed = jnp.dot(
        lax.all_gather(features, "feat", axis=1, tiled=True),
        weight_cols,
        preferred_element_type=jnp.float32,
    )
    projected = summed.astype(jnp.bfloat16)
    half_rows = send_rows.shape[2]
    slot_total = send_rows.shape[1]
    offsets = list(range(-REACH, 0)) + list(range(1, REACH + 1))
    packed_all = projected[send_rows[0].reshape(slot_total * half_rows)].reshape(
        slot_total, half_rows, column_count
    )
    received = []
    for slot_index, offset_value in enumerate(offsets):
        received.append(passed_along(packed_all[slot_index], "dom", offset_value))
    halo_block = jnp.concatenate(received, 0)
    owners = hub_ids // vertex_rows
    mine = owners == part_index
    local_index = jnp.clip(hub_ids - part_index * vertex_rows, 0, vertex_rows - 1)
    candidates = projected[local_index]
    hub_total = hub_ids.shape[0]
    positions = jnp.arange(hub_total, dtype=jnp.int32)
    earlier = (owners[:, None] == owners[None, :]) & (positions[:, None] > positions[None, :])
    ranks = jnp.sum(earlier.astype(jnp.int32), 1)
    selector = (
        mine[:, None] & (ranks[:, None] == jnp.arange(HUB_MOST, dtype=jnp.int32)[None, :])
    ).astype(jnp.bfloat16)
    slot_rows = lax.dot_general(
        selector, candidates, (((0,), (0,)), ((), ())), preferred_element_type=jnp.float32
    ).astype(jnp.bfloat16)
    gathered = lax.all_gather(slot_rows, "dom", axis=0, tiled=True)
    hub_block = gathered[owners * HUB_MOST + ranks]
    extended = jnp.concatenate([projected, halo_block, hub_block], 0)
    block_edge = tile_values.shape[1]
    blocks = extended.reshape(extended.shape[0] // block_edge, block_edge, column_count)
    products = jnp.einsum(
        "tij,tjc->tic", tile_values, blocks[tile_cols], preferred_element_type=jnp.float32
    )
    live_mask = jnp.arange(tile_values.shape[0], dtype=jnp.int32) < tile_count[0]
    block_count = vertex_rows // block_edge
    assignment = (
        (tile_rows[None, :] == jnp.arange(block_count, dtype=jnp.int32)[:, None])
        & live_mask[None, :]
    ).astype(jnp.float32)
    aggregate = jnp.einsum("rt,tic->ric", assignment, products, precision=lax.Precision.HIGHEST)
    activated = jnp.maximum(aggregate + out_bias[None, None, :], 0.0).astype(jnp.bfloat16)
    return activated.reshape(vertex_rows, column_count)

LANES = 128
GROUPS = 4
PLANE = 4
PIECES = 2
HELD = 1
OUTER_ORDER = (-1, 4, -3, 3, -2, 1, 2, -4)
INNER_ORDER = (-3, 4, 1, -2, 3, -4, 2, -1)
MESH = pl.DeviceIdType.MESH


def picked_rows(index, table_ref, groups):
    depth = table_ref.shape[0]
    group = index // depth
    within = index - group * depth
    positions = lax.broadcasted_iota(jnp.int32, (index.shape[0], depth), 1)
    chosen = (positions == within).astype(jnp.float32).astype(jnp.bfloat16)
    every = jnp.dot(chosen, table_ref[...], preferred_element_type=jnp.float32)
    width = table_ref.shape[1] // groups
    result = every[:, :width]
    for number in range(1, groups):
        part = every[:, number * width : (number + 1) * width]
        result = jnp.where(group == number, part, result)
    return result.astype(jnp.bfloat16)


def over_rows(left, right):
    dims = (((0,), (0,)), ((), ()))
    return lax.dot_general(left, right, dims, preferred_element_type=jnp.float32)


def exchange_kernel(
    count, features_hbm, weight_hbm, send_hbm, hub_hbm, extended_ref,
    features_ref, weight_ref, send_ref, hub_ref, load_sems,
    partial_ref, other_ref, total_ref, table_ref, ordered_ref, index_ref, packed_ref,
    own_hubs_ref, hubs_ref, near_hubs_ref, far_hubs_ref,
    feature_sems, send_sems, receive_sems, hub_send_sems, hub_receive_sems,
):
    part = lax.axis_index("dom")
    feat = lax.axis_index("feat")
    depth, vertex_rows = features_ref.shape
    width = extended_ref.shape[1]
    loads = []
    for number, (source, target) in enumerate(
        (
            (features_hbm, features_ref), (weight_hbm, weight_ref),
            (hub_hbm, hub_ref), (send_hbm, send_ref),
        )
    ):
        loads.append(pltpu.make_async_copy(source, target, load_sems.at[number]))
        loads[number].start()
    lines = count // PLANE
    line = part // PLANE
    place = part - line * PLANE
    group_rows = vertex_rows // GROUPS
    slots, half_rows = send_ref.shape
    chunk = half_rows // PIECES
    offsets = list(range(-REACH, 0)) + list(range(1, REACH + 1))
    hub_total = hub_ref.shape[1]
    halo_end = vertex_rows + slots * half_rows

    barrier = pltpu.get_barrier_semaphore()
    pl.semaphore_signal(barrier, inc=1, device_id=(part, 1 - feat), device_id_type=MESH)

    def greet(step, carry):
        peer = lax.rem(part + step * PLANE, count)
        pl.semaphore_signal(barrier, inc=1, device_id=(peer, feat), device_id_type=MESH)
        return carry

    lax.fori_loop(1, lines, greet, 0)
    greeted = lines
    for offset in offsets:
        if abs(offset) % PLANE != 0:
            target = part + offset
            inside = (target >= 0) & (target < count)
            greeted = greeted + inside.astype(jnp.int32)

            @pl.when(inside)
            def _():
                pl.semaphore_signal(
                    barrier, inc=1, device_id=(target, feat), device_id_type=MESH
                )

    outer = (place == 0) | (place == PLANE - 1)
    sign = jnp.where(place < PLANE // 2, 1, -1)
    ordered = [sign * jnp.where(outer, *pair) for pair in zip(OUTER_ORDER, INNER_ORDER)]
    ordered_slots = [
        jnp.where(offset < 0, offset + REACH, offset + REACH - 1) for offset in ordered
    ]

    loads[0].wait()
    loads[1].wait()
    own_depth = pl.ds(pl.multiple_of(feat * depth, 16), depth)
    own_columns = pl.ds(pl.multiple_of(feat * width, width), width)
    other_columns = pl.ds(pl.multiple_of((1 - feat) * width, width), width)
    partial_ref[...] = over_rows(weight_ref[own_depth, other_columns], features_ref[...])

    pl.semaphore_wait(barrier, greeted)

    exchanges = []
    for group in range(GROUPS):
        columns = pl.ds(group * group_rows, group_rows)
        exchanges.append(
            pltpu.make_async_remote_copy(
                src_ref=partial_ref.at[:, columns], dst_ref=other_ref.at[:, columns],
                send_sem=feature_sems.at[0, group], recv_sem=feature_sems.at[1, group],
                device_id=(part, 1 - feat), device_id_type=MESH,
            )
        )
        exchanges[group].start()
    total_ref[...] = over_rows(weight_ref[own_depth, own_columns], features_ref[...])
    loads[2].wait()
    hub_row = hub_ref[...]
    hub_col = jnp.transpose(jnp.broadcast_to(hub_row, (8, hub_total)))[:, :1]
    owner_row = hub_row // vertex_rows
    owner_col = hub_col // vertex_rows
    same = owner_row == owner_col
    first = lax.broadcasted_iota(jnp.int32, (hub_total, hub_total), 0)
    second = lax.broadcasted_iota(jnp.int32, (hub_total, hub_total), 1)
    rank_row = jnp.sum(jnp.where(same & (first < second), 1.0, 0.0), 0, keepdims=True)
    rank_col = jnp.sum(jnp.where(same & (second < first), 1.0, 0.0), 1, keepdims=True)
    rank_row = rank_row.astype(jnp.int32)
    rank_col = rank_col.astype(jnp.int32)
    ranks = lax.broadcasted_iota(jnp.int32, (HUB_MOST, hub_total), 0)
    chosen = (rank_row == ranks) & (owner_row == part)
    local_row = (hub_row - part * vertex_rows).astype(jnp.float32)
    own_index = jnp.sum(jnp.where(chosen, local_row, 0.0), 1, keepdims=True).astype(jnp.int32)
    loads[3].wait()
    for number, slot in enumerate(ordered_slots):
        ordered_ref[number : number + 1, :] = send_ref[pl.ds(slot, 1), :]
    index_ref[...] = jnp.transpose(ordered_ref[...])

    for group in range(GROUPS):
        rows = pl.ds(group * group_rows, group_rows)
        exchanges[group].wait_recv()
        projected = jnp.transpose(total_ref[:, rows] + other_ref[:, rows]).astype(jnp.bfloat16)
        extended_ref[rows, :] = projected
        table_ref[:, group * width : (group + 1) * width] = projected

    own_hubs = picked_rows(own_index, table_ref, GROUPS)
    own_hubs_ref[...] = own_hubs
    hub_home = (place * lines + line) * HUB_MOST
    hubs_ref[pl.ds(pl.multiple_of(hub_home, 16), HUB_MOST), :] = own_hubs

    def hub_copy(number, first, blocks, target, source_ref=None):
        rows = pl.ds(pl.multiple_of(first * HUB_MOST, 16), blocks * HUB_MOST)
        return pltpu.make_async_remote_copy(
            src_ref=hubs_ref.at[rows, :] if source_ref is None else source_ref,
            dst_ref=hubs_ref.at[rows, :],
            send_sem=hub_send_sems.at[number], recv_sem=hub_receive_sems.at[number],
            device_id=(target, feat), device_id_type=MESH,
        )

    side = lax.rem(place, 2)
    across = part + 1 - 2 * side
    across_place = place + 1 - 2 * side
    pair_place = place - side
    pair_side = place // 2
    far = part + 2 - 4 * pair_side

    def line_copy(step, from_line):
        target = lax.rem(part + step * PLANE, count)
        return hub_copy(1 + step, place * lines + from_line, 1, target, own_hubs_ref)

    for step in range(1, lines):
        line_copy(step, line).start()

    def halo_copy(number, slot, offset, piece):
        start = vertex_rows + slot * half_rows + piece * chunk
        rows = pl.ds(pl.multiple_of(start, 16), chunk)
        return pltpu.make_async_remote_copy(
            src_ref=packed_ref.at[number, piece * chunk : (piece + 1) * chunk, :],
            dst_ref=extended_ref.at[rows, :],
            send_sem=send_sems.at[number, piece], recv_sem=receive_sems.at[slot, piece],
            device_id=(lax.rem(part + offset + count, count), feat), device_id_type=MESH,
        )

    def present(number):
        target = part + ordered[number]
        return (target >= 0) & (target < count)

    def wait_sent(number, pieces):
        for piece in pieces:
            halo_copy(number, ordered_slots[number], ordered[number], piece).wait_send()

    early = range(PIECES - HELD)
    late = range(PIECES - HELD, PIECES)

    def gate(number, also=True):
        @pl.when(present(number) & also)
        def _():
            wait_sent(number, early)

    def pick(number):
        @pl.when(present(number))
        def _():
            for piece in range(PIECES):
                rows = pl.ds(piece * chunk, chunk)
                index = index_ref[rows, number : number + 1]
                packed_ref[number, rows, :] = picked_rows(index, table_ref, GROUPS)
                if number < 2:
                    halo_copy(number, ordered_slots[number], ordered[number], piece).start()

    def send(number, also=True):
        @pl.when(present(number) & also)
        def _():
            for piece in range(PIECES):
                halo_copy(number, ordered_slots[number], ordered[number], piece).start()

    inner = jnp.logical_not(outer)
    pick(0)
    pick(1)
    pick(2)
    for step in range(1, lines):
        line_copy(step, lax.rem(line - step + lines, lines)).wait_recv()
    hub_copy(0, place * lines, lines, across).start()
    pick(3)
    gate(0)
    send(2)
    send(3, inner)
    pick(4)
    pick(5)
    pick(6)
    pick(7)
    gate(2)
    send(3, outer)
    send(4)
    send(5)
    hub_copy(0, across_place * lines, lines, across).wait_recv()
    pair_rows = 2 * lines * HUB_MOST
    pair_start = pair_place * lines * HUB_MOST
    owner_line = owner_col // PLANE
    owner_place = owner_col - owner_line * PLANE
    within = (owner_place * lines + owner_line) * HUB_MOST + rank_col - pair_start
    positions = lax.broadcasted_iota(jnp.int32, (hub_total, pair_rows), 1)
    chosen = (positions == within).astype(jnp.float32).astype(jnp.bfloat16)
    pair_hubs = hubs_ref[pl.ds(pl.multiple_of(pair_start, 16), pair_rows), :]
    near_hubs = jnp.dot(chosen, pair_hubs, preferred_element_type=jnp.float32)
    near_hubs_ref[...] = near_hubs.astype(jnp.bfloat16)
    hub_exchange = pltpu.make_async_remote_copy(
        src_ref=near_hubs_ref, dst_ref=far_hubs_ref,
        send_sem=hub_send_sems.at[1], recv_sem=hub_receive_sems.at[1],
        device_id=(far, feat), device_id_type=MESH,
    )
    hub_exchange.start()
    gate(3)
    gate(4)
    send(6)
    send(7)

    for slot, offset in enumerate(offsets):
        source = part - offset

        @pl.when((source < 0) | (source >= count))
        def _():
            rows = pl.ds(vertex_rows + slot * half_rows, half_rows)
            extended_ref[rows, :] = jnp.zeros((half_rows, width), jnp.bfloat16)

    hub_exchange.wait_recv()
    hubs = near_hubs_ref[...].astype(jnp.float32) + far_hubs_ref[...].astype(jnp.float32)
    extended_ref[halo_end : halo_end + hub_total, :] = hubs.astype(jnp.bfloat16)
    for exchange in exchanges:
        exchange.wait_send()
    hub_copy(0, place * lines, lines, across).wait_send()
    hub_exchange.wait_send()
    for step in range(1, lines):
        line_copy(step, line).wait_send()
    for number in range(slots):
        gated = number in (0, 2, 3, 4)

        @pl.when(present(number))
        def _():
            wait_sent(number, late if gated else range(PIECES))

    for slot, offset in enumerate(offsets):
        source = part - offset

        @pl.when((source >= 0) & (source < count))
        def _():
            for piece in range(PIECES):
                halo_copy(0, slot, offset, piece).wait_recv()


def tiles_kernel(
    rows_in, cols_in, count_ref, values_ref, extended_ref, bias_ref, out_ref,
    total_ref, rows_ref, cols_ref, sems,
):
    loads = []
    for number, (source, target) in enumerate(
        ((rows_in, rows_ref), (cols_in, cols_ref))
    ):
        loads.append(pltpu.make_async_copy(source, target, sems.at[number]))
        loads[number].start()
    slots, edge, _ = values_ref.shape
    width = out_ref.shape[1]
    spare = out_ref.shape[0] // edge
    total_ref[...] = jnp.zeros_like(total_ref)
    for load in loads:
        load.wait()
    live = count_ref[0]
    together = math.gcd(slots, 12)

    def step(number, carry):
        products, places = [], []
        for inner in range(together):
            slot = number * together + inner
            block = pl.ds(pl.multiple_of(cols_ref[slot] * edge, edge), edge)
            places.append(jnp.where(slot < live, rows_ref[slot], spare))
            products.append(
                jnp.dot(values_ref[slot], extended_ref[block, :], preferred_element_type=jnp.float32)
            )
        for place, product in zip(places, products):
            total_ref[pl.ds(pl.multiple_of(place * edge, edge), edge), :] += product
        return carry

    lax.fori_loop(0, (live + together - 1) // together, step, 0)
    summed = total_ref[: out_ref.shape[0], :] + bias_ref[...]
    out_ref[...] = jnp.maximum(summed, 0.0).astype(jnp.bfloat16)


def local(
    features, weight, out_bias, tile_values, tile_rows, tile_cols, tile_count, send_rows, hub_ids
):
    width = out_bias.shape[0]
    vertex_rows, depth = features.shape
    count = lax.axis_size("dom")
    _, slots, half_rows = send_rows.shape
    hub_total = hub_ids.shape[0]
    edge = tile_values.shape[1]
    vmem = pl.BlockSpec(memory_space=pltpu.VMEM)
    extended_rows = vertex_rows + slots * half_rows + hub_total
    extended = pl.pallas_call(
        functools.partial(exchange_kernel, count),
        out_shape=jax.ShapeDtypeStruct((extended_rows, width), jnp.bfloat16),
        in_specs=[pl.BlockSpec(memory_space=pltpu.HBM)] * 4,
        out_specs=vmem,
        scratch_shapes=[
            pltpu.VMEM((depth, vertex_rows), jnp.bfloat16),
            pltpu.VMEM(weight.shape, jnp.bfloat16),
            pltpu.VMEM((slots, half_rows), jnp.int32),
            pltpu.VMEM((1, hub_total), jnp.int32),
            pltpu.SemaphoreType.DMA((4,)),
            pltpu.VMEM((width, vertex_rows), jnp.float32),
            pltpu.VMEM((width, vertex_rows), jnp.float32),
            pltpu.VMEM((width, vertex_rows), jnp.float32),
            pltpu.VMEM((vertex_rows // GROUPS, GROUPS * width), jnp.bfloat16),
            pltpu.VMEM((slots, half_rows), jnp.int32),
            pltpu.VMEM((half_rows, slots), jnp.int32),
            pltpu.VMEM((slots, half_rows, width), jnp.bfloat16),
            pltpu.VMEM((HUB_MOST, width), jnp.bfloat16),
            pltpu.VMEM((count * HUB_MOST, width), jnp.bfloat16),
            pltpu.VMEM((hub_total, width), jnp.bfloat16),
            pltpu.VMEM((hub_total, width), jnp.bfloat16),
            pltpu.SemaphoreType.DMA((2, GROUPS)),
            pltpu.SemaphoreType.DMA((slots, PIECES)),
            pltpu.SemaphoreType.DMA((slots, PIECES)),
            pltpu.SemaphoreType.DMA((count // PLANE + 1,)),
            pltpu.SemaphoreType.DMA((count // PLANE + 1,)),
        ],
        compiler_params=pltpu.CompilerParams(
            collective_id=0, has_side_effects=True, vmem_limit_bytes=32 << 20
        ),
    )(
        *[
            pltpu.with_memory_space_constraint(value, pltpu.HBM)
            for value in (jnp.transpose(features), weight, send_rows[0], hub_ids[None, :])
        ]
    )
    return pl.pallas_call(
        tiles_kernel,
        out_shape=jax.ShapeDtypeStruct((vertex_rows, width), jnp.bfloat16),
        in_specs=[vmem] * 2 + [pl.BlockSpec(memory_space=pltpu.SMEM)] + [vmem] * 3,
        out_specs=vmem,
        scratch_shapes=[
            pltpu.VMEM((vertex_rows + edge, width), jnp.float32),
            pltpu.SMEM(tile_rows.shape, jnp.int32),
            pltpu.SMEM(tile_cols.shape, jnp.int32),
            pltpu.SemaphoreType.DMA((2,)),
        ],
        compiler_params=pltpu.CompilerParams(vmem_limit_bytes=24 << 20),
    )(
        tile_rows,
        tile_cols,
        tile_count,
        tile_values,
        extended,
        out_bias[None, :],
    )


def solution(mesh):
    in_specs = (
        P("dom", "feat"),
        P(),
        P("feat"),
        P("dom", None, None),
        P("dom"),
        P("dom"),
        P("dom"),
        P("dom", None, None),
        P(),
    )
    out_specs = P("dom", "feat")

    def program(features, weight, out_bias, *rest):
        whole_lanes = out_bias.shape[0] % (LANES * mesh.shape["feat"]) == 0
        fits = mesh.shape["feat"] == 2 and mesh.shape["dom"] % PLANE == 0
        body = local if fits and whole_lanes else local_any
        return jax.shard_map(
            body, mesh=mesh, in_specs=in_specs, out_specs=out_specs, check_vma=False
        )(features, weight, out_bias, *rest)

    return program
```

```python
import functools
import math

import jax
import jax.numpy as jnp
from jax import lax
from jax.experimental import pallas as pl
from jax.experimental.pallas import tpu as pltpu
from jax.sharding import PartitionSpec as P

REACH = 4
HUB_MOST = 48


def passed_along(value, axis, steps):
    count = lax.axis_size(axis)
    initial, last = (max(0, -steps), min(count, count - steps))
    return lax.ppermute(value, axis, [(source, source + steps) for source in range(initial, last)])


def local_any(
    features, weight, out_bias, tile_values, tile_rows, tile_cols, tile_count, send_rows, hub_ids
):
    column_count = out_bias.shape[0]
    vertex_rows = features.shape[0]
    part_index = lax.axis_index("dom")
    feat_index = lax.axis_index("feat")
    weight_cols = lax.dynamic_slice_in_dim(weight, feat_index * column_count, column_count, 1)
    summed = jnp.dot(
        lax.all_gather(features, "feat", axis=1, tiled=True),
        weight_cols,
        preferred_element_type=jnp.float32,
    )
    projected = summed.astype(jnp.bfloat16)
    half_rows = send_rows.shape[2]
    slot_total = send_rows.shape[1]
    offsets = list(range(-REACH, 0)) + list(range(1, REACH + 1))
    packed_all = projected[send_rows[0].reshape(slot_total * half_rows)].reshape(
        slot_total, half_rows, column_count
    )
    received = []
    for slot_index, offset_value in enumerate(offsets):
        received.append(passed_along(packed_all[slot_index], "dom", offset_value))
    halo_block = jnp.concatenate(received, 0)
    owners = hub_ids // vertex_rows
    mine = owners == part_index
    local_index = jnp.clip(hub_ids - part_index * vertex_rows, 0, vertex_rows - 1)
    candidates = projected[local_index]
    hub_total = hub_ids.shape[0]
    positions = jnp.arange(hub_total, dtype=jnp.int32)
    earlier = (owners[:, None] == owners[None, :]) & (positions[:, None] > positions[None, :])
    ranks = jnp.sum(earlier.astype(jnp.int32), 1)
    selector = (
        mine[:, None] & (ranks[:, None] == jnp.arange(HUB_MOST, dtype=jnp.int32)[None, :])
    ).astype(jnp.bfloat16)
    slot_rows = lax.dot_general(
        selector, candidates, (((0,), (0,)), ((), ())), preferred_element_type=jnp.float32
    ).astype(jnp.bfloat16)
    gathered = lax.all_gather(slot_rows, "dom", axis=0, tiled=True)
    hub_block = gathered[owners * HUB_MOST + ranks]
    extended = jnp.concatenate([projected, halo_block, hub_block], 0)
    block_edge = tile_values.shape[1]
    blocks = extended.reshape(extended.shape[0] // block_edge, block_edge, column_count)
    products = jnp.einsum(
        "tij,tjc->tic", tile_values, blocks[tile_cols], preferred_element_type=jnp.float32
    )
    live_mask = jnp.arange(tile_values.shape[0], dtype=jnp.int32) < tile_count[0]
    block_count = vertex_rows // block_edge
    assignment = (
        (tile_rows[None, :] == jnp.arange(block_count, dtype=jnp.int32)[:, None])
        & live_mask[None, :]
    ).astype(jnp.float32)
    aggregate = jnp.einsum("rt,tic->ric", assignment, products, precision=lax.Precision.HIGHEST)
    activated = jnp.maximum(aggregate + out_bias[None, None, :], 0.0).astype(jnp.bfloat16)
    return activated.reshape(vertex_rows, column_count)

LANES = 128
GROUPS = 4
PLANE = 4
PIECES = 4
HELD = 1
EARLY = 5
OUTER_ORDER = (-1, 4, -3, 3, -2, 1, 2, -4)
INNER_ORDER = (-3, 4, 1, -2, 3, -4, 2, -1)
MESH = pl.DeviceIdType.MESH


def picked_rows(index, table_ref, groups):
    depth = table_ref.shape[0]
    group = index // depth
    within = index - group * depth
    positions = lax.broadcasted_iota(jnp.int32, (index.shape[0], depth), 1)
    chosen = (positions == within).astype(jnp.float32).astype(jnp.bfloat16)
    every = jnp.dot(chosen, table_ref[...], preferred_element_type=jnp.float32)
    width = table_ref.shape[1] // groups
    result = every[:, :width]
    for number in range(1, groups):
        part = every[:, number * width : (number + 1) * width]
        result = jnp.where(group == number, part, result)
    return result.astype(jnp.bfloat16)


def over_rows(left, right):
    dims = (((0,), (0,)), ((), ()))
    return lax.dot_general(left, right, dims, preferred_element_type=jnp.float32)


def arrange_tiles(
    live, rows, cols, own_blocks, slot_blocks, present_slots, early_slots, early_meta_ref, late_ref
):
    total = rows.shape[1]
    square = (total, total)
    down = lax.broadcasted_iota(jnp.int32, square, 0)
    along = lax.broadcasted_iota(jnp.int32, square, 1)
    lane = lax.broadcasted_iota(jnp.int32, rows.shape, 1)
    early = (cols < own_blocks).astype(jnp.int32)
    is_live = (lane < live).astype(jnp.int32)
    for number, (present, flag) in enumerate(zip(present_slots, early_slots)):
        start = own_blocks + number * slot_blocks
        inside = ((cols >= start) & (cols < start + slot_blocks)).astype(jnp.int32)
        early = early + inside * flag.astype(jnp.int32)
        is_live = is_live * (1 - inside * (1 - present.astype(jnp.int32)))
    early = early * is_live
    late = is_live - early

    def upright(row):
        return jnp.transpose(jnp.broadcast_to(row, (8, total)))[:, :1]

    def places_of(key, key_col):
        before = (key_col < key) | ((key_col == key) & (down < along))
        return upright(jnp.sum(before.astype(jnp.int32), 0, keepdims=True))

    def moved(places, column, shift=0):
        return jnp.sum(jnp.where(places + shift == along, column, 0), 0, keepdims=True)

    rows_col, cols_col = upright(rows), upright(cols)
    slot_col = down[:, :1]
    last = jnp.int32(1 << 20)
    early_key = jnp.where(early > 0, rows, last)
    early_col = jnp.where(upright(early) > 0, rows_col, last)
    places = places_of(early_key, early_col)
    key_sorted = moved(places, early_col)
    key_before = moved(places, early_col, 1)
    same = (key_sorted == key_before) & (lane > 0)
    counted = jnp.sum((early_col == along).astype(jnp.int32), 0, keepdims=True)
    ended = jnp.sum((early_col <= along).astype(jnp.int32), 0, keepdims=True) - 1
    early_meta_ref[0:1, :] = moved(places, slot_col)
    early_meta_ref[1:2, :] = moved(places, cols_col)
    early_meta_ref[2:3, :] = same.astype(jnp.int32)
    early_meta_ref[3:4, :] = jnp.maximum(ended, 0)
    early_meta_ref[4:5, :] = counted
    early_meta_ref[5:8, :] = jnp.zeros((3, total), jnp.int32)
    late_key = 1 - late
    places = places_of(late_key, upright(late_key))
    late_ref[0:1, :] = moved(places, slot_col)
    late_ref[1:2, :] = moved(places, rows_col)
    late_ref[2:3, :] = moved(places, cols_col)
    late_spread = jnp.broadcast_to(upright(late), square)
    late_ref[3:4, :] = jnp.sum(late_spread, 0, keepdims=True)
    late_ref[4:8, :] = jnp.zeros((4, total), jnp.int32)


def exchange_kernel(
    count, features_hbm, weight_hbm, send_hbm, hub_hbm, rows_hbm, cols_hbm, values_hbm, live_ref,
    extended_ref, values_ref, early_total_ref, late_smem,
    features_ref, weight_ref, send_ref, hub_ref, rows_ref, cols_ref, load_sems,
    early_ref, early_meta_ref, late_ref, early_smem, sums_ref,
    partial_ref, other_ref, total_ref, table_ref, ordered_ref, index_ref, packed_ref,
    own_hubs_ref, hubs_ref, near_hubs_ref, far_hubs_ref,
    feature_sems, send_sems, receive_sems, hub_send_sems, hub_receive_sems,
):
    part = lax.axis_index("dom")
    feat = lax.axis_index("feat")
    depth, vertex_rows = features_ref.shape
    width = extended_ref.shape[2]
    loads = []
    group_rows = vertex_rows // GROUPS
    feature_parts = [pl.ds(group * group_rows, group_rows) for group in range(GROUPS)]
    for number, (source, target) in enumerate(
        [(weight_hbm, weight_ref)]
        + [(features_hbm.at[:, rows], features_ref.at[:, rows]) for rows in feature_parts]
        + [(hub_hbm, hub_ref), (send_hbm, send_ref), (rows_hbm, rows_ref), (cols_hbm, cols_ref)]
    ):
        loads.append(pltpu.make_async_copy(source, target, load_sems.at[number]))
        loads[number].start()
    lines = count // PLANE
    line = part // PLANE
    place = part - line * PLANE
    slots, half_rows = send_ref.shape
    chunk = half_rows // PIECES
    offsets = list(range(-REACH, 0)) + list(range(1, REACH + 1))
    hub_total = hub_ref.shape[1]
    tile_slots, edge, _ = values_ref.shape
    own_blocks = vertex_rows // edge
    slot_blocks = half_rows // edge
    piece_blocks = chunk // edge
    hub_block = own_blocks + slots * slot_blocks

    barrier = pltpu.get_barrier_semaphore()
    pl.semaphore_signal(barrier, inc=1, device_id=(part, 1 - feat), device_id_type=MESH)

    def greet(step, carry):
        peer = lax.rem(part + step * PLANE, count)
        pl.semaphore_signal(barrier, inc=1, device_id=(peer, feat), device_id_type=MESH)
        return carry

    lax.fori_loop(1, lines, greet, 0)
    greeted = lines
    for offset in offsets:
        if abs(offset) % PLANE != 0:
            target = part + offset
            inside = (target >= 0) & (target < count)
            greeted = greeted + inside.astype(jnp.int32)

            @pl.when(inside)
            def _():
                pl.semaphore_signal(
                    barrier, inc=1, device_id=(target, feat), device_id_type=MESH
                )

    outer = (place == 0) | (place == PLANE - 1)
    sign = jnp.where(place < PLANE // 2, 1, -1)
    ordered = [sign * jnp.where(outer, *pair) for pair in zip(OUTER_ORDER, INNER_ORDER)]
    ordered_slots = [
        jnp.where(offset < 0, offset + REACH, offset + REACH - 1) for offset in ordered
    ]

    def arriving(offset):
        source = part - offset
        return (source >= 0) & (source < count)

    def arrives_early(offset):
        source_place = lax.rem(place - offset + 2 * PLANE, PLANE)
        found = source_place < 0
        for number, (order, turn) in enumerate(
            ((OUTER_ORDER, 1), (INNER_ORDER, 1), (INNER_ORDER, -1), (OUTER_ORDER, -1))
        ):
            if turn * offset in order[:EARLY]:
                found = found | (source_place == number)
        return found & arriving(offset)

    loads[0].wait()
    own_depth = pl.ds(pl.multiple_of(feat * depth, 16), depth)
    own_columns = pl.ds(pl.multiple_of(feat * width, width), width)
    other_columns = pl.ds(pl.multiple_of((1 - feat) * width, width), width)
    exchanges = []
    for group, rows in enumerate(feature_parts):
        loads[1 + group].wait()
        partial_ref[:, rows] = over_rows(
            weight_ref[own_depth, other_columns], features_ref[:, rows]
        )
        if group == 0:
            pl.semaphore_wait(barrier, greeted)
        exchanges.append(
            pltpu.make_async_remote_copy(
                src_ref=partial_ref.at[:, rows], dst_ref=other_ref.at[:, rows],
                send_sem=feature_sems.at[0, group], recv_sem=feature_sems.at[1, group],
                device_id=(part, 1 - feat), device_id_type=MESH,
            )
        )
        exchanges[group].start()
    values_load = pltpu.make_async_copy(values_hbm, values_ref, load_sems.at[5 + GROUPS])
    values_load.start()
    total_ref[...] = over_rows(weight_ref[own_depth, own_columns], features_ref[...])
    loads[1 + GROUPS].wait()
    hub_row = hub_ref[...]
    hub_col = jnp.transpose(jnp.broadcast_to(hub_row, (8, hub_total)))[:, :1]
    owner_row = hub_row // vertex_rows
    owner_col = hub_col // vertex_rows
    same = owner_row == owner_col
    first = lax.broadcasted_iota(jnp.int32, (hub_total, hub_total), 0)
    second = lax.broadcasted_iota(jnp.int32, (hub_total, hub_total), 1)
    rank_row = jnp.sum(jnp.where(same & (first < second), 1.0, 0.0), 0, keepdims=True)
    rank_col = jnp.sum(jnp.where(same & (second < first), 1.0, 0.0), 1, keepdims=True)
    rank_row = rank_row.astype(jnp.int32)
    rank_col = rank_col.astype(jnp.int32)
    ranks = lax.broadcasted_iota(jnp.int32, (HUB_MOST, hub_total), 0)
    chosen = (rank_row == ranks) & (owner_row == part)
    local_row = (hub_row - part * vertex_rows).astype(jnp.float32)
    own_index = jnp.sum(jnp.where(chosen, local_row, 0.0), 1, keepdims=True).astype(jnp.int32)
    loads[2 + GROUPS].wait()
    for number, slot in enumerate(ordered_slots):
        ordered_ref[number : number + 1, :] = send_ref[pl.ds(slot, 1), :]
    index_ref[...] = jnp.transpose(ordered_ref[...])

    for group in range(GROUPS):
        rows = pl.ds(group * group_rows, group_rows)
        exchanges[group].wait_recv()
        projected = jnp.transpose(total_ref[:, rows] + other_ref[:, rows]).astype(jnp.bfloat16)
        group_blocks = group_rows // edge
        early_ref[group * group_blocks : (group + 1) * group_blocks] = projected.reshape(
            group_blocks, edge, width
        )
        table_ref[:, group * width : (group + 1) * width] = projected

    def hub_copy(number, first, blocks, target, source_ref=None):
        rows = pl.ds(pl.multiple_of(first * HUB_MOST, 16), blocks * HUB_MOST)
        return pltpu.make_async_remote_copy(
            src_ref=hubs_ref.at[rows, :] if source_ref is None else source_ref,
            dst_ref=hubs_ref.at[rows, :],
            send_sem=hub_send_sems.at[number], recv_sem=hub_receive_sems.at[number],
            device_id=(target, feat), device_id_type=MESH,
        )

    side = lax.rem(place, 2)
    across = part + 1 - 2 * side
    across_place = place + 1 - 2 * side
    pair_place = place - side
    pair_side = place // 2
    far = part + 2 - 4 * pair_side

    def line_copy(step, from_line):
        target = lax.rem(part + step * PLANE, count)
        return hub_copy(1 + step, place * lines + from_line, 1, target, own_hubs_ref)

    def halo_copy(number, slot, offset, piece):
        landing_ref = early_ref if number < EARLY else extended_ref
        start = own_blocks + slot * slot_blocks + piece * piece_blocks
        blocks = pl.ds(start, piece_blocks)
        return pltpu.make_async_remote_copy(
            src_ref=packed_ref.at[number, pl.ds(piece * piece_blocks, piece_blocks)],
            dst_ref=landing_ref.at[blocks],
            send_sem=send_sems.at[number, piece], recv_sem=receive_sems.at[slot, piece],
            device_id=(lax.rem(part + offset + count, count), feat), device_id_type=MESH,
        )

    def present(number):
        target = part + ordered[number]
        return (target >= 0) & (target < count)

    def wait_sent(number, pieces):
        for piece in pieces:
            halo_copy(number, ordered_slots[number], ordered[number], piece).wait_send()

    early = range(PIECES - HELD)
    late = range(PIECES - HELD, PIECES)

    def gate(number, also=True):
        @pl.when(present(number) & also)
        def _():
            wait_sent(number, early)

    def pick(number):
        @pl.when(present(number))
        def _():
            for piece in range(PIECES):
                rows = pl.ds(piece * chunk, chunk)
                index = index_ref[rows, number : number + 1]
                packed_ref[number, pl.ds(piece * piece_blocks, piece_blocks)] = picked_rows(
                    index, table_ref, GROUPS
                ).reshape(piece_blocks, edge, width)
                if number < 2:
                    halo_copy(number, ordered_slots[number], ordered[number], piece).start()

    def send(number, also=True, pieces=range(PIECES)):
        @pl.when(present(number) & also)
        def _():
            for piece in pieces:
                halo_copy(number, ordered_slots[number], ordered[number], piece).start()

    inner = jnp.logical_not(outer)
    own_hubs = picked_rows(own_index, table_ref, GROUPS)
    own_hubs_ref[...] = own_hubs
    hub_home = (place * lines + line) * HUB_MOST
    hubs_ref[pl.ds(pl.multiple_of(hub_home, 16), HUB_MOST), :] = own_hubs
    for step in range(1, lines):
        line_copy(step, line).start()
    pick(0)
    pick(1)
    pick(2)
    pick(3)
    gate(0)
    send(2)
    send(3, inner)
    pick(4)
    pick(5)
    pick(6)
    pick(7)
    for step in range(1, lines):
        line_copy(step, lax.rem(line - step + lines, lines)).wait_recv()
    loads[3 + GROUPS].wait()
    loads[4 + GROUPS].wait()
    arrange_tiles(
        live_ref[0], rows_ref[...], cols_ref[...], own_blocks, slot_blocks,
        [arriving(offset) for offset in offsets],
        [arrives_early(offset) for offset in offsets], early_meta_ref, late_ref,
    )
    meta_copy = pltpu.make_async_copy(early_meta_ref, early_smem, load_sems.at[6 + GROUPS])
    meta_copy.start()
    late_copy = pltpu.make_async_copy(late_ref, late_smem, load_sems.at[7 + GROUPS])
    late_copy.start()
    gate(2)
    send(3, outer)
    send(4)
    hub_copy(0, place * lines, lines, across).start()
    send(5)
    gate(3)
    gate(4)
    send(6, pieces=range(PIECES - 1))
    send(7)
    hub_copy(0, across_place * lines, lines, across).wait_recv()
    pair_rows = 2 * lines * HUB_MOST
    pair_start = pair_place * lines * HUB_MOST
    owner_line = owner_col // PLANE
    owner_place = owner_col - owner_line * PLANE
    within = (owner_place * lines + owner_line) * HUB_MOST + rank_col - pair_start
    positions = lax.broadcasted_iota(jnp.int32, (hub_total, pair_rows), 1)
    chosen = (positions == within).astype(jnp.float32).astype(jnp.bfloat16)
    pair_hubs = hubs_ref[pl.ds(pl.multiple_of(pair_start, 16), pair_rows), :]
    near_hubs = jnp.dot(chosen, pair_hubs, preferred_element_type=jnp.float32)
    near_hubs_ref[...] = near_hubs.astype(jnp.bfloat16)
    hub_exchange = pltpu.make_async_remote_copy(
        src_ref=near_hubs_ref, dst_ref=far_hubs_ref,
        send_sem=hub_send_sems.at[1], recv_sem=hub_receive_sems.at[1],
        device_id=(far, feat), device_id_type=MESH,
    )
    hub_exchange.start()
    send(6, pieces=range(PIECES - 1, PIECES))

    for slot, offset in enumerate(offsets):

        @pl.when(arrives_early(offset))
        def _():
            for piece in range(PIECES):
                halo_copy(0, slot, offset, piece).wait_recv()

    values_load.wait()
    meta_copy.wait()
    late_copy.wait()
    together = math.gcd(tile_slots, 12)

    def step(number, running):
        for inner in range(together):
            entry = number * together + inner
            product = jnp.dot(
                values_ref[early_smem[0, entry]], early_ref[early_smem[1, entry]],
                preferred_element_type=jnp.float32,
            )
            kept = jnp.broadcast_to(early_smem[2, entry], running.shape) > 0
            running = jnp.where(kept, running, 0.0) + product
            sums_ref[entry] = running
        return running

    lax.fori_loop(0, tile_slots // together, step, jnp.zeros((edge, width), jnp.float32))
    for block in range(vertex_rows // edge):
        summed = sums_ref[early_smem[3, block]]
        kept = jnp.broadcast_to(early_smem[4, block], summed.shape) > 0
        early_total_ref[block * edge : (block + 1) * edge, :] = jnp.where(kept, summed, 0.0)

    hub_exchange.wait_recv()
    hubs = near_hubs_ref[...].astype(jnp.float32) + far_hubs_ref[...].astype(jnp.float32)
    extended_ref[hub_block:] = hubs.astype(jnp.bfloat16).reshape(hub_total // edge, edge, width)
    for exchange in exchanges:
        exchange.wait_send()
    hub_copy(0, place * lines, lines, across).wait_send()
    hub_exchange.wait_send()
    for step in range(1, lines):
        line_copy(step, line).wait_send()
    for number in range(slots):
        gated = number in (0, 2, 3, 4)

        @pl.when(present(number))
        def _():
            wait_sent(number, late if gated else range(PIECES))

    for slot, offset in enumerate(offsets):

        @pl.when(arriving(offset) & jnp.logical_not(arrives_early(offset)))
        def _():
            for piece in range(PIECES):
                halo_copy(EARLY, slot, offset, piece).wait_recv()


def tiles_kernel(
    late_ref, values_ref, extended_ref, start_ref, bias_ref, out_ref, total_ref
):
    slots, edge, _ = values_ref.shape
    spare = out_ref.shape[0] // edge
    total_ref[: out_ref.shape[0], :] = start_ref[...]
    total_ref[out_ref.shape[0] :, :] = jnp.zeros((edge, out_ref.shape[1]), jnp.float32)
    live = late_ref[3, 0]
    together = math.gcd(slots, 12)

    def step(number, carry):
        products, places = [], []
        for inner in range(together):
            entry = number * together + inner
            places.append(jnp.where(entry < live, late_ref[1, entry], spare))
            products.append(
                jnp.dot(
                    values_ref[late_ref[0, entry]], extended_ref[late_ref[2, entry]],
                    preferred_element_type=jnp.float32,
                )
            )
        for place, product in zip(places, products):
            total_ref[pl.ds(pl.multiple_of(place * edge, edge), edge), :] += product
        return carry

    lax.fori_loop(0, (live + together - 1) // together, step, 0)
    summed = total_ref[: out_ref.shape[0], :] + bias_ref[...]
    out_ref[...] = jnp.maximum(summed, 0.0).astype(jnp.bfloat16)


def local(
    features, weight, out_bias, tile_values, tile_rows, tile_cols, tile_count, send_rows, hub_ids
):
    width = out_bias.shape[0]
    vertex_rows, depth = features.shape
    count = lax.axis_size("dom")
    _, slots, half_rows = send_rows.shape
    hub_total = hub_ids.shape[0]
    edge = tile_values.shape[1]
    vmem = pl.BlockSpec(memory_space=pltpu.VMEM)
    blocks = (vertex_rows + slots * half_rows + hub_total) // edge
    tile_slots = tile_values.shape[0]
    hbm = pl.BlockSpec(memory_space=pltpu.HBM)
    smem = pl.BlockSpec(memory_space=pltpu.SMEM)
    extended, values, early_total, late = pl.pallas_call(
        functools.partial(exchange_kernel, count),
        out_shape=[
            jax.ShapeDtypeStruct((blocks, edge, width), jnp.bfloat16),
            jax.ShapeDtypeStruct(tile_values.shape, jnp.bfloat16),
            jax.ShapeDtypeStruct((vertex_rows, width), jnp.float32),
            pltpu.SMEM((8, tile_slots), jnp.int32),
        ],
        in_specs=[hbm] * 7 + [smem],
        out_specs=[vmem] * 3 + [smem],
        scratch_shapes=[
            pltpu.VMEM((depth, vertex_rows), jnp.bfloat16),
            pltpu.VMEM(weight.shape, jnp.bfloat16),
            pltpu.VMEM((slots, half_rows), jnp.int32),
            pltpu.VMEM((1, hub_total), jnp.int32),
            pltpu.VMEM((1, tile_slots), jnp.int32),
            pltpu.VMEM((1, tile_slots), jnp.int32),
            pltpu.SemaphoreType.DMA((8 + GROUPS,)),
            pltpu.VMEM((blocks, edge, width), jnp.bfloat16),
            pltpu.VMEM((8, tile_slots), jnp.int32),
            pltpu.VMEM((8, tile_slots), jnp.int32),
            pltpu.SMEM((8, tile_slots), jnp.int32),
            pltpu.VMEM((tile_slots, edge, width), jnp.float32),
            pltpu.VMEM((width, vertex_rows), jnp.float32),
            pltpu.VMEM((width, vertex_rows), jnp.float32),
            pltpu.VMEM((width, vertex_rows), jnp.float32),
            pltpu.VMEM((vertex_rows // GROUPS, GROUPS * width), jnp.bfloat16),
            pltpu.VMEM((slots, half_rows), jnp.int32),
            pltpu.VMEM((half_rows, slots), jnp.int32),
            pltpu.VMEM((slots, half_rows // edge, edge, width), jnp.bfloat16),
            pltpu.VMEM((HUB_MOST, width), jnp.bfloat16),
            pltpu.VMEM((count * HUB_MOST, width), jnp.bfloat16),
            pltpu.VMEM((hub_total, width), jnp.bfloat16),
            pltpu.VMEM((hub_total, width), jnp.bfloat16),
            pltpu.SemaphoreType.DMA((2, GROUPS)),
            pltpu.SemaphoreType.DMA((slots, PIECES)),
            pltpu.SemaphoreType.DMA((slots, PIECES)),
            pltpu.SemaphoreType.DMA((count // PLANE + 1,)),
            pltpu.SemaphoreType.DMA((count // PLANE + 1,)),
        ],
        compiler_params=pltpu.CompilerParams(
            collective_id=0, has_side_effects=True, vmem_limit_bytes=32 << 20
        ),
    )(
        *[
            pltpu.with_memory_space_constraint(value, pltpu.HBM)
            for value in (
                jnp.transpose(features), weight, send_rows[0], hub_ids[None, :],
                tile_rows[None, :], tile_cols[None, :], tile_values,
            )
        ],
        tile_count,
    )
    return pl.pallas_call(
        tiles_kernel,
        out_shape=jax.ShapeDtypeStruct((vertex_rows, width), jnp.bfloat16),
        in_specs=[smem] + [vmem] * 4,
        out_specs=vmem,
        scratch_shapes=[
            pltpu.VMEM((vertex_rows + edge, width), jnp.float32),
        ],
        compiler_params=pltpu.CompilerParams(vmem_limit_bytes=24 << 20),
    )(late, values, extended, early_total, out_bias[None, :])


def solution(mesh):
    in_specs = (
        P("dom", "feat"),
        P(),
        P("feat"),
        P("dom", None, None),
        P("dom"),
        P("dom"),
        P("dom"),
        P("dom", None, None),
        P(),
    )
    out_specs = P("dom", "feat")

    def program(features, weight, out_bias, *rest):
        whole_lanes = out_bias.shape[0] % (LANES * mesh.shape["feat"]) == 0
        tile_values, send_rows, hub_ids = rest[0], rest[4], rest[5]
        edge = tile_values.shape[1]
        fits = mesh.shape["feat"] == 2 and mesh.shape["dom"] % PLANE == 0
        fits = fits and features.shape[0] % (mesh.shape["dom"] * GROUPS * edge) == 0
        fits = fits and send_rows.shape[2] % (PIECES * edge) == 0 and hub_ids.shape[0] % edge == 0
        body = local if fits and whole_lanes else local_any
        return jax.shard_map(
            body, mesh=mesh, in_specs=in_specs, out_specs=out_specs, check_vma=False
        )(features, weight, out_bias, *rest)

    return program
```

```python
import functools
import math

import jax
import jax.numpy as jnp
from jax import lax
from jax.experimental import pallas as pl
from jax.experimental.pallas import tpu as pltpu
from jax.sharding import PartitionSpec as P

REACH = 4
HUB_MOST = 48


def passed_along(value, axis, steps):
    count = lax.axis_size(axis)
    initial, last = (max(0, -steps), min(count, count - steps))
    return lax.ppermute(value, axis, [(source, source + steps) for source in range(initial, last)])


def local_any(
    features, weight, out_bias, tile_values, tile_rows, tile_cols, tile_count, send_rows, hub_ids
):
    column_count = out_bias.shape[0]
    vertex_rows = features.shape[0]
    part_index = lax.axis_index("dom")
    feat_index = lax.axis_index("feat")
    weight_cols = lax.dynamic_slice_in_dim(weight, feat_index * column_count, column_count, 1)
    summed = jnp.dot(
        lax.all_gather(features, "feat", axis=1, tiled=True),
        weight_cols,
        preferred_element_type=jnp.float32,
    )
    projected = summed.astype(jnp.bfloat16)
    half_rows = send_rows.shape[2]
    slot_total = send_rows.shape[1]
    offsets = list(range(-REACH, 0)) + list(range(1, REACH + 1))
    packed_all = projected[send_rows[0].reshape(slot_total * half_rows)].reshape(
        slot_total, half_rows, column_count
    )
    received = []
    for slot_index, offset_value in enumerate(offsets):
        received.append(passed_along(packed_all[slot_index], "dom", offset_value))
    halo_block = jnp.concatenate(received, 0)
    owners = hub_ids // vertex_rows
    mine = owners == part_index
    local_index = jnp.clip(hub_ids - part_index * vertex_rows, 0, vertex_rows - 1)
    candidates = projected[local_index]
    hub_total = hub_ids.shape[0]
    positions = jnp.arange(hub_total, dtype=jnp.int32)
    earlier = (owners[:, None] == owners[None, :]) & (positions[:, None] > positions[None, :])
    ranks = jnp.sum(earlier.astype(jnp.int32), 1)
    selector = (
        mine[:, None] & (ranks[:, None] == jnp.arange(HUB_MOST, dtype=jnp.int32)[None, :])
    ).astype(jnp.bfloat16)
    slot_rows = lax.dot_general(
        selector, candidates, (((0,), (0,)), ((), ())), preferred_element_type=jnp.float32
    ).astype(jnp.bfloat16)
    gathered = lax.all_gather(slot_rows, "dom", axis=0, tiled=True)
    hub_block = gathered[owners * HUB_MOST + ranks]
    extended = jnp.concatenate([projected, halo_block, hub_block], 0)
    block_edge = tile_values.shape[1]
    blocks = extended.reshape(extended.shape[0] // block_edge, block_edge, column_count)
    products = jnp.einsum(
        "tij,tjc->tic", tile_values, blocks[tile_cols], preferred_element_type=jnp.float32
    )
    live_mask = jnp.arange(tile_values.shape[0], dtype=jnp.int32) < tile_count[0]
    block_count = vertex_rows // block_edge
    assignment = (
        (tile_rows[None, :] == jnp.arange(block_count, dtype=jnp.int32)[:, None])
        & live_mask[None, :]
    ).astype(jnp.float32)
    aggregate = jnp.einsum("rt,tic->ric", assignment, products, precision=lax.Precision.HIGHEST)
    activated = jnp.maximum(aggregate + out_bias[None, None, :], 0.0).astype(jnp.bfloat16)
    return activated.reshape(vertex_rows, column_count)

LANES = 128
GROUPS = 4
PLANE = 4
PIECES = 4
HELD = 1
EARLY = 5
OUTER_ORDER = (-1, 4, -3, 3, -2, 1, 2, -4)
INNER_ORDER = (-3, 4, 1, -2, 3, -4, 2, -1)
MESH = pl.DeviceIdType.MESH


def picked_rows(index, table_ref, groups):
    depth = table_ref.shape[0]
    group = index // depth
    within = index - group * depth
    positions = lax.broadcasted_iota(jnp.int32, (index.shape[0], depth), 1)
    chosen = (positions == within).astype(jnp.float32).astype(jnp.bfloat16)
    every = jnp.dot(chosen, table_ref[...], preferred_element_type=jnp.float32)
    width = table_ref.shape[1] // groups
    result = every[:, :width]
    for number in range(1, groups):
        part = every[:, number * width : (number + 1) * width]
        result = jnp.where(group == number, part, result)
    return result.astype(jnp.bfloat16)


def over_rows(left, right):
    dims = (((0,), (0,)), ((), ()))
    return lax.dot_general(left, right, dims, preferred_element_type=jnp.float32)


def arrange_tiles(
    live, rows, cols, own_blocks, slot_blocks, present_slots, early_slots, early_meta_ref, late_ref
):
    total = rows.shape[1]
    square = (total, total)
    down = lax.broadcasted_iota(jnp.int32, square, 0)
    along = lax.broadcasted_iota(jnp.int32, square, 1)
    lane = lax.broadcasted_iota(jnp.int32, rows.shape, 1)
    early = (cols < own_blocks).astype(jnp.int32)
    is_live = (lane < live).astype(jnp.int32)
    for number, (present, flag) in enumerate(zip(present_slots, early_slots)):
        start = own_blocks + number * slot_blocks
        inside = ((cols >= start) & (cols < start + slot_blocks)).astype(jnp.int32)
        early = early + inside * flag.astype(jnp.int32)
        is_live = is_live * (1 - inside * (1 - present.astype(jnp.int32)))
    early = early * is_live
    late = is_live - early

    def upright(row):
        return jnp.transpose(jnp.broadcast_to(row, (8, total)))[:, :1]

    def places_of(key, key_col):
        before = (key_col < key) | ((key_col == key) & (down < along))
        return upright(jnp.sum(before.astype(jnp.int32), 0, keepdims=True))

    def moved(places, column, shift=0):
        return jnp.sum(jnp.where(places + shift == along, column, 0), 0, keepdims=True)

    rows_col, cols_col = upright(rows), upright(cols)
    slot_col = down[:, :1]
    last = jnp.int32(1 << 20)
    early_key = jnp.where(early > 0, rows, last)
    early_col = jnp.where(upright(early) > 0, rows_col, last)
    places = places_of(early_key, early_col)
    key_sorted = moved(places, early_col)
    key_before = moved(places, early_col, 1)
    same = (key_sorted == key_before) & (lane > 0)
    counted = jnp.sum((early_col == along).astype(jnp.int32), 0, keepdims=True)
    ended = jnp.sum((early_col <= along).astype(jnp.int32), 0, keepdims=True) - 1
    early_meta_ref[0:1, :] = moved(places, slot_col)
    early_meta_ref[1:2, :] = moved(places, cols_col)
    early_meta_ref[2:3, :] = same.astype(jnp.int32)
    early_meta_ref[3:4, :] = jnp.maximum(ended, 0)
    early_meta_ref[4:5, :] = counted
    early_meta_ref[5:8, :] = jnp.zeros((3, total), jnp.int32)
    late_key = 1 - late
    places = places_of(late_key, upright(late_key))
    late_ref[0:1, :] = moved(places, slot_col)
    late_ref[1:2, :] = moved(places, rows_col)
    late_ref[2:3, :] = moved(places, cols_col)
    late_spread = jnp.broadcast_to(upright(late), square)
    late_ref[3:4, :] = jnp.sum(late_spread, 0, keepdims=True)
    late_ref[4:8, :] = jnp.zeros((4, total), jnp.int32)


def exchange_kernel(
    count, features_hbm, weight_hbm, send_hbm, hub_hbm, rows_hbm, cols_hbm, values_hbm, live_ref,
    extended_ref, values_ref, early_total_ref, late_smem,
    features_ref, weight_ref, send_ref, hub_ref, rows_ref, cols_ref, load_sems,
    early_ref, early_meta_ref, late_ref, early_smem, sums_ref,
    partial_ref, other_ref, total_ref, table_ref, ordered_ref, index_ref, packed_ref,
    own_hubs_ref, hubs_ref, near_hubs_ref, far_hubs_ref,
    feature_sems, send_sems, receive_sems, hub_send_sems, hub_receive_sems,
):
    part = lax.axis_index("dom")
    feat = lax.axis_index("feat")
    depth, vertex_rows = features_ref.shape
    width = extended_ref.shape[2]
    loads = []
    group_rows = vertex_rows // GROUPS
    feature_parts = [pl.ds(group * group_rows, group_rows) for group in range(GROUPS)]
    for number, (source, target) in enumerate(
        [(weight_hbm, weight_ref)]
        + [(features_hbm.at[:, rows], features_ref.at[:, rows]) for rows in feature_parts]
        + [(hub_hbm, hub_ref), (send_hbm, send_ref), (rows_hbm, rows_ref), (cols_hbm, cols_ref)]
    ):
        loads.append(pltpu.make_async_copy(source, target, load_sems.at[number]))
        loads[number].start()
    lines = count // PLANE
    line = part // PLANE
    place = part - line * PLANE
    slots, half_rows = send_ref.shape
    chunk = half_rows // PIECES
    offsets = list(range(-REACH, 0)) + list(range(1, REACH + 1))
    hub_total = hub_ref.shape[1]
    tile_slots, edge, _ = values_ref.shape
    own_blocks = vertex_rows // edge
    slot_blocks = half_rows // edge
    piece_blocks = chunk // edge
    hub_block = own_blocks + slots * slot_blocks

    barrier = pltpu.get_barrier_semaphore()
    pl.semaphore_signal(barrier, inc=1, device_id=(part, 1 - feat), device_id_type=MESH)

    def greet(step, carry):
        peer = lax.rem(part + step * PLANE, count)
        pl.semaphore_signal(barrier, inc=1, device_id=(peer, feat), device_id_type=MESH)
        return carry

    lax.fori_loop(1, lines, greet, 0)
    greeted = lines
    for offset in offsets:
        if abs(offset) % PLANE != 0:
            target = part + offset
            inside = (target >= 0) & (target < count)
            greeted = greeted + inside.astype(jnp.int32)

            @pl.when(inside)
            def _():
                pl.semaphore_signal(
                    barrier, inc=1, device_id=(target, feat), device_id_type=MESH
                )

    outer = (place == 0) | (place == PLANE - 1)
    sign = jnp.where(place < PLANE // 2, 1, -1)
    ordered = [sign * jnp.where(outer, *pair) for pair in zip(OUTER_ORDER, INNER_ORDER)]
    ordered_slots = [
        jnp.where(offset < 0, offset + REACH, offset + REACH - 1) for offset in ordered
    ]

    def arriving(offset):
        source = part - offset
        return (source >= 0) & (source < count)

    def arrives_early(offset):
        source_place = lax.rem(place - offset + 2 * PLANE, PLANE)
        found = source_place < 0
        for number, (order, turn) in enumerate(
            ((OUTER_ORDER, 1), (INNER_ORDER, 1), (INNER_ORDER, -1), (OUTER_ORDER, -1))
        ):
            if turn * offset in order[:EARLY]:
                found = found | (source_place == number)
        return found & arriving(offset)

    loads[0].wait()
    own_depth = pl.ds(pl.multiple_of(feat * depth, 16), depth)
    own_columns = pl.ds(pl.multiple_of(feat * width, width), width)
    other_columns = pl.ds(pl.multiple_of((1 - feat) * width, width), width)
    exchanges = []
    for group, rows in enumerate(feature_parts):
        loads[1 + group].wait()
        partial_ref[:, rows] = over_rows(
            weight_ref[own_depth, other_columns], features_ref[:, rows]
        ).astype(jnp.bfloat16)
        if group == 0:
            pl.semaphore_wait(barrier, greeted)
        exchanges.append(
            pltpu.make_async_remote_copy(
                src_ref=partial_ref.at[:, rows], dst_ref=other_ref.at[:, rows],
                send_sem=feature_sems.at[0, group], recv_sem=feature_sems.at[1, group],
                device_id=(part, 1 - feat), device_id_type=MESH,
            )
        )
        exchanges[group].start()
    values_load = pltpu.make_async_copy(values_hbm, values_ref, load_sems.at[5 + GROUPS])
    values_load.start()
    total_ref[...] = over_rows(weight_ref[own_depth, own_columns], features_ref[...])
    loads[1 + GROUPS].wait()
    hub_row = hub_ref[...]
    hub_col = jnp.transpose(jnp.broadcast_to(hub_row, (8, hub_total)))[:, :1]
    owner_row = hub_row // vertex_rows
    owner_col = hub_col // vertex_rows
    same = owner_row == owner_col
    first = lax.broadcasted_iota(jnp.int32, (hub_total, hub_total), 0)
    second = lax.broadcasted_iota(jnp.int32, (hub_total, hub_total), 1)
    rank_row = jnp.sum(jnp.where(same & (first < second), 1.0, 0.0), 0, keepdims=True)
    rank_col = jnp.sum(jnp.where(same & (second < first), 1.0, 0.0), 1, keepdims=True)
    rank_row = rank_row.astype(jnp.int32)
    rank_col = rank_col.astype(jnp.int32)
    ranks = lax.broadcasted_iota(jnp.int32, (HUB_MOST, hub_total), 0)
    chosen = (rank_row == ranks) & (owner_row == part)
    local_row = (hub_row - part * vertex_rows).astype(jnp.float32)
    own_index = jnp.sum(jnp.where(chosen, local_row, 0.0), 1, keepdims=True).astype(jnp.int32)
    loads[2 + GROUPS].wait()
    for number, slot in enumerate(ordered_slots):
        ordered_ref[number : number + 1, :] = send_ref[pl.ds(slot, 1), :]
    index_ref[...] = jnp.transpose(ordered_ref[...])

    for group in range(GROUPS):
        rows = pl.ds(group * group_rows, group_rows)
        exchanges[group].wait_recv()
        projected = jnp.transpose(total_ref[:, rows] + other_ref[:, rows]).astype(jnp.bfloat16)
        group_blocks = group_rows // edge
        early_ref[group * group_blocks : (group + 1) * group_blocks] = projected.reshape(
            group_blocks, edge, width
        )
        table_ref[:, group * width : (group + 1) * width] = projected

    def hub_copy(number, first, blocks, target, source_ref=None):
        rows = pl.ds(pl.multiple_of(first * HUB_MOST, 16), blocks * HUB_MOST)
        return pltpu.make_async_remote_copy(
            src_ref=hubs_ref.at[rows, :] if source_ref is None else source_ref,
            dst_ref=hubs_ref.at[rows, :],
            send_sem=hub_send_sems.at[number], recv_sem=hub_receive_sems.at[number],
            device_id=(target, feat), device_id_type=MESH,
        )

    side = lax.rem(place, 2)
    across = part + 1 - 2 * side
    across_place = place + 1 - 2 * side
    pair_place = place - side
    pair_side = place // 2
    far = part + 2 - 4 * pair_side

    def line_copy(step, from_line):
        target = lax.rem(part + step * PLANE, count)
        return hub_copy(1 + step, place * lines + from_line, 1, target, own_hubs_ref)

    def halo_copy(number, slot, offset, piece):
        landing_ref = early_ref if number < EARLY else extended_ref
        start = own_blocks + slot * slot_blocks + piece * piece_blocks
        blocks = pl.ds(start, piece_blocks)
        return pltpu.make_async_remote_copy(
            src_ref=packed_ref.at[number, pl.ds(piece * piece_blocks, piece_blocks)],
            dst_ref=landing_ref.at[blocks],
            send_sem=send_sems.at[number, piece], recv_sem=receive_sems.at[slot, piece],
            device_id=(lax.rem(part + offset + count, count), feat), device_id_type=MESH,
        )

    def present(number):
        target = part + ordered[number]
        return (target >= 0) & (target < count)

    def wait_sent(number, pieces):
        for piece in pieces:
            halo_copy(number, ordered_slots[number], ordered[number], piece).wait_send()

    early = range(PIECES - HELD)
    late = range(PIECES - HELD, PIECES)

    def gate(number, also=True):
        @pl.when(present(number) & also)
        def _():
            wait_sent(number, early)

    def pick(number):
        @pl.when(present(number))
        def _():
            for piece in range(PIECES):
                rows = pl.ds(piece * chunk, chunk)
                index = index_ref[rows, number : number + 1]
                packed_ref[number, pl.ds(piece * piece_blocks, piece_blocks)] = picked_rows(
                    index, table_ref, GROUPS
                ).reshape(piece_blocks, edge, width)
                if number < 2:
                    halo_copy(number, ordered_slots[number], ordered[number], piece).start()

    def send(number, also=True, pieces=range(PIECES)):
        @pl.when(present(number) & also)
        def _():
            for piece in pieces:
                halo_copy(number, ordered_slots[number], ordered[number], piece).start()

    inner = jnp.logical_not(outer)
    own_hubs = picked_rows(own_index, table_ref, GROUPS)
    own_hubs_ref[...] = own_hubs
    hub_home = (place * lines + line) * HUB_MOST
    hubs_ref[pl.ds(pl.multiple_of(hub_home, 16), HUB_MOST), :] = own_hubs
    for step in range(1, lines):
        line_copy(step, line).start()
    pick(0)
    pick(1)
    pick(2)
    pick(3)
    gate(0)
    send(2)
    send(3, inner)
    pick(4)
    pick(5)
    pick(6)
    pick(7)
    for step in range(1, lines):
        line_copy(step, lax.rem(line - step + lines, lines)).wait_recv()
    loads[3 + GROUPS].wait()
    loads[4 + GROUPS].wait()
    arrange_tiles(
        live_ref[0], rows_ref[...], cols_ref[...], own_blocks, slot_blocks,
        [arriving(offset) for offset in offsets],
        [arrives_early(offset) for offset in offsets], early_meta_ref, late_ref,
    )
    meta_copy = pltpu.make_async_copy(early_meta_ref, early_smem, load_sems.at[6 + GROUPS])
    meta_copy.start()
    late_copy = pltpu.make_async_copy(late_ref, late_smem, load_sems.at[7 + GROUPS])
    late_copy.start()
    gate(2)
    send(3, outer)
    send(4)
    hub_copy(0, place * lines, lines, across).start()
    send(5)
    gate(3)
    gate(4)
    send(6)
    send(7)
    hub_copy(0, across_place * lines, lines, across).wait_recv()
    pair_rows = 2 * lines * HUB_MOST
    pair_start = pair_place * lines * HUB_MOST
    owner_line = owner_col // PLANE
    owner_place = owner_col - owner_line * PLANE
    within = (owner_place * lines + owner_line) * HUB_MOST + rank_col - pair_start
    positions = lax.broadcasted_iota(jnp.int32, (hub_total, pair_rows), 1)
    chosen = (positions == within).astype(jnp.float32).astype(jnp.bfloat16)
    pair_hubs = hubs_ref[pl.ds(pl.multiple_of(pair_start, 16), pair_rows), :]
    near_hubs = jnp.dot(chosen, pair_hubs, preferred_element_type=jnp.float32)
    near_hubs_ref[...] = near_hubs.astype(jnp.bfloat16)
    hub_exchange = pltpu.make_async_remote_copy(
        src_ref=near_hubs_ref, dst_ref=far_hubs_ref,
        send_sem=hub_send_sems.at[1], recv_sem=hub_receive_sems.at[1],
        device_id=(far, feat), device_id_type=MESH,
    )
    hub_exchange.start()

    for slot, offset in enumerate(offsets):

        @pl.when(arrives_early(offset))
        def _():
            for piece in range(PIECES):
                halo_copy(0, slot, offset, piece).wait_recv()

    values_load.wait()
    meta_copy.wait()
    late_copy.wait()
    together = math.gcd(tile_slots, 12)

    def step(number, running):
        for inner in range(together):
            entry = number * together + inner
            product = jnp.dot(
                values_ref[early_smem[0, entry]], early_ref[early_smem[1, entry]],
                preferred_element_type=jnp.float32,
            )
            kept = jnp.broadcast_to(early_smem[2, entry], running.shape) > 0
            running = jnp.where(kept, running, 0.0) + product
            sums_ref[entry] = running
        return running

    lax.fori_loop(0, tile_slots // together, step, jnp.zeros((edge, width), jnp.float32))
    for block in range(vertex_rows // edge):
        summed = sums_ref[early_smem[3, block]]
        kept = jnp.broadcast_to(early_smem[4, block], summed.shape) > 0
        early_total_ref[block * edge : (block + 1) * edge, :] = jnp.where(kept, summed, 0.0)

    hub_exchange.wait_recv()
    hubs = near_hubs_ref[...].astype(jnp.float32) + far_hubs_ref[...].astype(jnp.float32)
    extended_ref[hub_block:] = hubs.astype(jnp.bfloat16).reshape(hub_total // edge, edge, width)
    for exchange in exchanges:
        exchange.wait_send()
    hub_copy(0, place * lines, lines, across).wait_send()
    hub_exchange.wait_send()
    for step in range(1, lines):
        line_copy(step, line).wait_send()
    for number in range(slots):
        gated = number in (0, 2, 3, 4)

        @pl.when(present(number))
        def _():
            wait_sent(number, late if gated else range(PIECES))

    for slot, offset in enumerate(offsets):

        @pl.when(arriving(offset) & jnp.logical_not(arrives_early(offset)))
        def _():
            for piece in range(PIECES):
                halo_copy(EARLY, slot, offset, piece).wait_recv()


def tiles_kernel(
    late_ref, values_ref, extended_ref, start_ref, bias_ref, out_ref, total_ref
):
    slots, edge, _ = values_ref.shape
    spare = out_ref.shape[0] // edge
    total_ref[: out_ref.shape[0], :] = start_ref[...]
    total_ref[out_ref.shape[0] :, :] = jnp.zeros((edge, out_ref.shape[1]), jnp.float32)
    live = late_ref[3, 0]
    together = math.gcd(slots, 12)

    def step(number, carry):
        products, places = [], []
        for inner in range(together):
            entry = number * together + inner
            places.append(jnp.where(entry < live, late_ref[1, entry], spare))
            products.append(
                jnp.dot(
                    values_ref[late_ref[0, entry]], extended_ref[late_ref[2, entry]],
                    preferred_element_type=jnp.float32,
                )
            )
        for place, product in zip(places, products):
            total_ref[pl.ds(pl.multiple_of(place * edge, edge), edge), :] += product
        return carry

    lax.fori_loop(0, (live + together - 1) // together, step, 0)
    summed = total_ref[: out_ref.shape[0], :] + bias_ref[...]
    out_ref[...] = jnp.maximum(summed, 0.0).astype(jnp.bfloat16)


def local(
    features, weight, out_bias, tile_values, tile_rows, tile_cols, tile_count, send_rows, hub_ids
):
    width = out_bias.shape[0]
    vertex_rows, depth = features.shape
    count = lax.axis_size("dom")
    _, slots, half_rows = send_rows.shape
    hub_total = hub_ids.shape[0]
    edge = tile_values.shape[1]
    vmem = pl.BlockSpec(memory_space=pltpu.VMEM)
    blocks = (vertex_rows + slots * half_rows + hub_total) // edge
    tile_slots = tile_values.shape[0]
    hbm = pl.BlockSpec(memory_space=pltpu.HBM)
    smem = pl.BlockSpec(memory_space=pltpu.SMEM)
    extended, values, early_total, late = pl.pallas_call(
        functools.partial(exchange_kernel, count),
        out_shape=[
            jax.ShapeDtypeStruct((blocks, edge, width), jnp.bfloat16),
            jax.ShapeDtypeStruct(tile_values.shape, jnp.bfloat16),
            jax.ShapeDtypeStruct((vertex_rows, width), jnp.float32),
            pltpu.SMEM((8, tile_slots), jnp.int32),
        ],
        in_specs=[hbm] * 7 + [smem],
        out_specs=[vmem] * 3 + [smem],
        scratch_shapes=[
            pltpu.VMEM((depth, vertex_rows), jnp.bfloat16),
            pltpu.VMEM(weight.shape, jnp.bfloat16),
            pltpu.VMEM((slots, half_rows), jnp.int32),
            pltpu.VMEM((1, hub_total), jnp.int32),
            pltpu.VMEM((1, tile_slots), jnp.int32),
            pltpu.VMEM((1, tile_slots), jnp.int32),
            pltpu.SemaphoreType.DMA((8 + GROUPS,)),
            pltpu.VMEM((blocks, edge, width), jnp.bfloat16),
            pltpu.VMEM((8, tile_slots), jnp.int32),
            pltpu.VMEM((8, tile_slots), jnp.int32),
            pltpu.SMEM((8, tile_slots), jnp.int32),
            pltpu.VMEM((tile_slots, edge, width), jnp.float32),
            pltpu.VMEM((width, vertex_rows), jnp.bfloat16),
            pltpu.VMEM((width, vertex_rows), jnp.bfloat16),
            pltpu.VMEM((width, vertex_rows), jnp.float32),
            pltpu.VMEM((vertex_rows // GROUPS, GROUPS * width), jnp.bfloat16),
            pltpu.VMEM((slots, half_rows), jnp.int32),
            pltpu.VMEM((half_rows, slots), jnp.int32),
            pltpu.VMEM((slots, half_rows // edge, edge, width), jnp.bfloat16),
            pltpu.VMEM((HUB_MOST, width), jnp.bfloat16),
            pltpu.VMEM((count * HUB_MOST, width), jnp.bfloat16),
            pltpu.VMEM((hub_total, width), jnp.bfloat16),
            pltpu.VMEM((hub_total, width), jnp.bfloat16),
            pltpu.SemaphoreType.DMA((2, GROUPS)),
            pltpu.SemaphoreType.DMA((slots, PIECES)),
            pltpu.SemaphoreType.DMA((slots, PIECES)),
            pltpu.SemaphoreType.DMA((count // PLANE + 1,)),
            pltpu.SemaphoreType.DMA((count // PLANE + 1,)),
        ],
        compiler_params=pltpu.CompilerParams(
            collective_id=0, has_side_effects=True, vmem_limit_bytes=32 << 20
        ),
    )(
        *[
            pltpu.with_memory_space_constraint(value, pltpu.HBM)
            for value in (
                jnp.transpose(features), weight, send_rows[0], hub_ids[None, :],
                tile_rows[None, :], tile_cols[None, :], tile_values,
            )
        ],
        tile_count,
    )
    return pl.pallas_call(
        tiles_kernel,
        out_shape=jax.ShapeDtypeStruct((vertex_rows, width), jnp.bfloat16),
        in_specs=[smem] + [vmem] * 4,
        out_specs=vmem,
        scratch_shapes=[
            pltpu.VMEM((vertex_rows + edge, width), jnp.float32),
        ],
        compiler_params=pltpu.CompilerParams(vmem_limit_bytes=24 << 20),
    )(late, values, extended, early_total, out_bias[None, :])


def solution(mesh):
    in_specs = (
        P("dom", "feat"),
        P(),
        P("feat"),
        P("dom", None, None),
        P("dom"),
        P("dom"),
        P("dom"),
        P("dom", None, None),
        P(),
    )
    out_specs = P("dom", "feat")

    def program(features, weight, out_bias, *rest):
        whole_lanes = out_bias.shape[0] % (LANES * mesh.shape["feat"]) == 0
        tile_values, send_rows, hub_ids = rest[0], rest[4], rest[5]
        edge = tile_values.shape[1]
        fits = mesh.shape["feat"] == 2 and mesh.shape["dom"] % PLANE == 0
        fits = fits and features.shape[0] % (mesh.shape["dom"] * GROUPS * edge) == 0
        fits = fits and send_rows.shape[2] % (PIECES * edge) == 0 and hub_ids.shape[0] % edge == 0
        body = local if fits and whole_lanes else local_any
        return jax.shard_map(
            body, mesh=mesh, in_specs=in_specs, out_specs=out_specs, check_vma=False
        )(features, weight, out_bias, *rest)

    return program
```

```python
import functools
import math

import jax
import jax.numpy as jnp
from jax import lax
from jax.experimental import pallas as pl
from jax.experimental.pallas import tpu as pltpu
from jax.sharding import PartitionSpec as P

REACH = 4
HUB_MOST = 48


def passed_along(value, axis, steps):
    count = lax.axis_size(axis)
    initial, last = (max(0, -steps), min(count, count - steps))
    return lax.ppermute(value, axis, [(source, source + steps) for source in range(initial, last)])


def local_any(
    features, weight, out_bias, tile_values, tile_rows, tile_cols, tile_count, send_rows, hub_ids
):
    column_count = out_bias.shape[0]
    vertex_rows = features.shape[0]
    part_index = lax.axis_index("dom")
    feat_index = lax.axis_index("feat")
    weight_cols = lax.dynamic_slice_in_dim(weight, feat_index * column_count, column_count, 1)
    summed = jnp.dot(
        lax.all_gather(features, "feat", axis=1, tiled=True),
        weight_cols,
        preferred_element_type=jnp.float32,
    )
    projected = summed.astype(jnp.bfloat16)
    half_rows = send_rows.shape[2]
    slot_total = send_rows.shape[1]
    offsets = list(range(-REACH, 0)) + list(range(1, REACH + 1))
    packed_all = projected[send_rows[0].reshape(slot_total * half_rows)].reshape(
        slot_total, half_rows, column_count
    )
    received = []
    for slot_index, offset_value in enumerate(offsets):
        received.append(passed_along(packed_all[slot_index], "dom", offset_value))
    halo_block = jnp.concatenate(received, 0)
    owners = hub_ids // vertex_rows
    mine = owners == part_index
    local_index = jnp.clip(hub_ids - part_index * vertex_rows, 0, vertex_rows - 1)
    candidates = projected[local_index]
    hub_total = hub_ids.shape[0]
    positions = jnp.arange(hub_total, dtype=jnp.int32)
    earlier = (owners[:, None] == owners[None, :]) & (positions[:, None] > positions[None, :])
    ranks = jnp.sum(earlier.astype(jnp.int32), 1)
    selector = (
        mine[:, None] & (ranks[:, None] == jnp.arange(HUB_MOST, dtype=jnp.int32)[None, :])
    ).astype(jnp.bfloat16)
    slot_rows = lax.dot_general(
        selector, candidates, (((0,), (0,)), ((), ())), preferred_element_type=jnp.float32
    ).astype(jnp.bfloat16)
    gathered = lax.all_gather(slot_rows, "dom", axis=0, tiled=True)
    hub_block = gathered[owners * HUB_MOST + ranks]
    extended = jnp.concatenate([projected, halo_block, hub_block], 0)
    block_edge = tile_values.shape[1]
    blocks = extended.reshape(extended.shape[0] // block_edge, block_edge, column_count)
    products = jnp.einsum(
        "tij,tjc->tic", tile_values, blocks[tile_cols], preferred_element_type=jnp.float32
    )
    live_mask = jnp.arange(tile_values.shape[0], dtype=jnp.int32) < tile_count[0]
    block_count = vertex_rows // block_edge
    assignment = (
        (tile_rows[None, :] == jnp.arange(block_count, dtype=jnp.int32)[:, None])
        & live_mask[None, :]
    ).astype(jnp.float32)
    aggregate = jnp.einsum("rt,tic->ric", assignment, products, precision=lax.Precision.HIGHEST)
    activated = jnp.maximum(aggregate + out_bias[None, None, :], 0.0).astype(jnp.bfloat16)
    return activated.reshape(vertex_rows, column_count)

LANES = 128
GROUPS = 4
PLANE = 4
PIECES = 4
HELD = 1
EARLY = 5
OUTER_ORDER = (-1, 4, -3, 3, -2, 1, 2, -4)
INNER_ORDER = (-3, 4, 1, -2, 3, -4, 2, -1)
MESH = pl.DeviceIdType.MESH


def picked_rows(index, table_ref, groups):
    depth = table_ref.shape[0]
    group = index // depth
    within = index - group * depth
    positions = lax.broadcasted_iota(jnp.int32, (index.shape[0], depth), 1)
    chosen = (positions == within).astype(jnp.float32).astype(jnp.bfloat16)
    every = jnp.dot(chosen, table_ref[...], preferred_element_type=jnp.float32)
    width = table_ref.shape[1] // groups
    result = every[:, :width]
    for number in range(1, groups):
        part = every[:, number * width : (number + 1) * width]
        result = jnp.where(group == number, part, result)
    return result.astype(jnp.bfloat16)


def over_rows(left, right):
    dims = (((0,), (0,)), ((), ()))
    return lax.dot_general(left, right, dims, preferred_element_type=jnp.float32)


def arrange_tiles(
    live, rows, cols, own_blocks, slot_blocks, present_slots, early_slots, early_meta_ref, late_ref
):
    total = rows.shape[1]
    square = (total, total)
    down = lax.broadcasted_iota(jnp.int32, square, 0)
    along = lax.broadcasted_iota(jnp.int32, square, 1)
    lane = lax.broadcasted_iota(jnp.int32, rows.shape, 1)
    early = (cols < own_blocks).astype(jnp.int32)
    is_live = (lane < live).astype(jnp.int32)
    for number, (present, flag) in enumerate(zip(present_slots, early_slots)):
        start = own_blocks + number * slot_blocks
        inside = ((cols >= start) & (cols < start + slot_blocks)).astype(jnp.int32)
        early = early + inside * flag.astype(jnp.int32)
        is_live = is_live * (1 - inside * (1 - present.astype(jnp.int32)))
    early = early * is_live
    late = is_live - early

    def upright(row):
        return jnp.transpose(jnp.broadcast_to(row, (8, total)))[:, :1]

    def places_of(key, key_col):
        before = (key_col < key) | ((key_col == key) & (down < along))
        return upright(jnp.sum(before.astype(jnp.int32), 0, keepdims=True))

    def moved(places, column, shift=0):
        return jnp.sum(jnp.where(places + shift == along, column, 0), 0, keepdims=True)

    rows_col, cols_col = upright(rows), upright(cols)
    slot_col = down[:, :1]
    last = jnp.int32(1 << 20)
    early_key = jnp.where(early > 0, rows, last)
    early_col = jnp.where(upright(early) > 0, rows_col, last)
    places = places_of(early_key, early_col)
    key_sorted = moved(places, early_col)
    key_before = moved(places, early_col, 1)
    same = (key_sorted == key_before) & (lane > 0)
    counted = jnp.sum((early_col == along).astype(jnp.int32), 0, keepdims=True)
    ended = jnp.sum((early_col <= along).astype(jnp.int32), 0, keepdims=True) - 1
    early_meta_ref[0:1, :] = moved(places, slot_col)
    early_meta_ref[1:2, :] = moved(places, cols_col)
    early_meta_ref[2:3, :] = same.astype(jnp.int32)
    early_meta_ref[3:4, :] = jnp.maximum(ended, 0)
    early_meta_ref[4:5, :] = counted
    early_meta_ref[5:8, :] = jnp.zeros((3, total), jnp.int32)
    late_key = 1 - late
    places = places_of(late_key, upright(late_key))
    late_ref[0:1, :] = moved(places, slot_col)
    late_ref[1:2, :] = moved(places, rows_col)
    late_ref[2:3, :] = moved(places, cols_col)
    late_spread = jnp.broadcast_to(upright(late), square)
    late_ref[3:4, :] = jnp.sum(late_spread, 0, keepdims=True)
    late_ref[4:8, :] = jnp.zeros((4, total), jnp.int32)


def exchange_kernel(
    count, features_hbm, weight_hbm, send_hbm, hub_hbm, rows_hbm, cols_hbm, values_hbm, live_ref,
    extended_ref, values_ref, early_total_ref, late_smem,
    features_ref, weight_ref, send_ref, hub_ref, rows_ref, cols_ref, load_sems,
    early_ref, early_meta_ref, late_ref, early_smem, sums_ref,
    partial_ref, other_ref, total_ref, table_ref, ordered_ref, index_ref, packed_ref,
    own_hubs_ref, hubs_ref, near_hubs_ref, far_hubs_ref,
    feature_sems, send_sems, receive_sems, hub_send_sems, hub_receive_sems,
):
    part = lax.axis_index("dom")
    feat = lax.axis_index("feat")
    depth, vertex_rows = features_ref.shape
    width = extended_ref.shape[2]
    loads = []
    group_rows = vertex_rows // GROUPS
    feature_parts = [pl.ds(group * group_rows, group_rows) for group in range(GROUPS)]
    for number, (source, target) in enumerate(
        [(weight_hbm, weight_ref)]
        + [(features_hbm.at[:, rows], features_ref.at[:, rows]) for rows in feature_parts]
        + [(hub_hbm, hub_ref), (send_hbm, send_ref), (rows_hbm, rows_ref), (cols_hbm, cols_ref)]
    ):
        loads.append(pltpu.make_async_copy(source, target, load_sems.at[number]))
        loads[number].start()
    lines = count // PLANE
    line = part // PLANE
    place = part - line * PLANE
    slots, half_rows = send_ref.shape
    chunk = half_rows // PIECES
    offsets = list(range(-REACH, 0)) + list(range(1, REACH + 1))
    hub_total = hub_ref.shape[1]
    tile_slots, edge, _ = values_ref.shape
    own_blocks = vertex_rows // edge
    slot_blocks = half_rows // edge
    piece_blocks = chunk // edge
    hub_block = own_blocks + slots * slot_blocks

    barrier = pltpu.get_barrier_semaphore()
    pl.semaphore_signal(barrier, inc=1, device_id=(part, 1 - feat), device_id_type=MESH)

    def greet(step, carry):
        peer = lax.rem(part + step * PLANE, count)
        pl.semaphore_signal(barrier, inc=1, device_id=(peer, feat), device_id_type=MESH)
        return carry

    lax.fori_loop(1, lines, greet, 0)
    greeted = lines
    for offset in offsets:
        if abs(offset) % PLANE != 0:
            target = part + offset
            inside = (target >= 0) & (target < count)
            greeted = greeted + inside.astype(jnp.int32)

            @pl.when(inside)
            def _():
                pl.semaphore_signal(
                    barrier, inc=1, device_id=(target, feat), device_id_type=MESH
                )

    outer = (place == 0) | (place == PLANE - 1)
    sign = jnp.where(place < PLANE // 2, 1, -1)
    ordered = [sign * jnp.where(outer, *pair) for pair in zip(OUTER_ORDER, INNER_ORDER)]
    ordered_slots = [
        jnp.where(offset < 0, offset + REACH, offset + REACH - 1) for offset in ordered
    ]

    def arriving(offset):
        source = part - offset
        return (source >= 0) & (source < count)

    def arrives_early(offset):
        source_place = lax.rem(place - offset + 2 * PLANE, PLANE)
        found = source_place < 0
        for number, (order, turn) in enumerate(
            ((OUTER_ORDER, 1), (INNER_ORDER, 1), (INNER_ORDER, -1), (OUTER_ORDER, -1))
        ):
            if turn * offset in order[:EARLY]:
                found = found | (source_place == number)
        return found & arriving(offset)

    loads[0].wait()
    own_depth = pl.ds(pl.multiple_of(feat * depth, 16), depth)
    own_columns = pl.ds(pl.multiple_of(feat * width, width), width)
    other_columns = pl.ds(pl.multiple_of((1 - feat) * width, width), width)
    exchanges = []
    for group, rows in enumerate(feature_parts):
        loads[1 + group].wait()
        partial_ref[:, rows] = over_rows(
            weight_ref[own_depth, other_columns], features_ref[:, rows]
        ).astype(jnp.bfloat16)

    pl.semaphore_wait(barrier, greeted)

    for group, rows in enumerate(feature_parts):
        exchanges.append(
            pltpu.make_async_remote_copy(
                src_ref=partial_ref.at[:, rows], dst_ref=other_ref.at[:, rows],
                send_sem=feature_sems.at[0, group], recv_sem=feature_sems.at[1, group],
                device_id=(part, 1 - feat), device_id_type=MESH,
            )
        )
        exchanges[group].start()
    values_load = pltpu.make_async_copy(values_hbm, values_ref, load_sems.at[5 + GROUPS])
    values_load.start()
    total_ref[...] = over_rows(weight_ref[own_depth, own_columns], features_ref[...])
    loads[1 + GROUPS].wait()
    hub_row = hub_ref[...]
    hub_col = jnp.transpose(jnp.broadcast_to(hub_row, (8, hub_total)))[:, :1]
    owner_row = hub_row // vertex_rows
    owner_col = hub_col // vertex_rows
    same = owner_row == owner_col
    first = lax.broadcasted_iota(jnp.int32, (hub_total, hub_total), 0)
    second = lax.broadcasted_iota(jnp.int32, (hub_total, hub_total), 1)
    rank_row = jnp.sum(jnp.where(same & (first < second), 1.0, 0.0), 0, keepdims=True)
    rank_col = jnp.sum(jnp.where(same & (second < first), 1.0, 0.0), 1, keepdims=True)
    rank_row = rank_row.astype(jnp.int32)
    rank_col = rank_col.astype(jnp.int32)
    ranks = lax.broadcasted_iota(jnp.int32, (HUB_MOST, hub_total), 0)
    chosen = (rank_row == ranks) & (owner_row == part)
    local_row = (hub_row - part * vertex_rows).astype(jnp.float32)
    own_index = jnp.sum(jnp.where(chosen, local_row, 0.0), 1, keepdims=True).astype(jnp.int32)
    loads[2 + GROUPS].wait()
    for number, slot in enumerate(ordered_slots):
        ordered_ref[number : number + 1, :] = send_ref[pl.ds(slot, 1), :]
    index_ref[...] = jnp.transpose(ordered_ref[...])

    for group in range(GROUPS):
        rows = pl.ds(group * group_rows, group_rows)
        exchanges[group].wait_recv()
        projected = jnp.transpose(total_ref[:, rows] + other_ref[:, rows]).astype(jnp.bfloat16)
        group_blocks = group_rows // edge
        early_ref[group * group_blocks : (group + 1) * group_blocks] = projected.reshape(
            group_blocks, edge, width
        )
        table_ref[:, group * width : (group + 1) * width] = projected

    def hub_copy(number, first, blocks, target, source_ref=None):
        rows = pl.ds(pl.multiple_of(first * HUB_MOST, 16), blocks * HUB_MOST)
        return pltpu.make_async_remote_copy(
            src_ref=hubs_ref.at[rows, :] if source_ref is None else source_ref,
            dst_ref=hubs_ref.at[rows, :],
            send_sem=hub_send_sems.at[number], recv_sem=hub_receive_sems.at[number],
            device_id=(target, feat), device_id_type=MESH,
        )

    side = lax.rem(place, 2)
    across = part + 1 - 2 * side
    across_place = place + 1 - 2 * side
    pair_place = place - side
    pair_side = place // 2
    far = part + 2 - 4 * pair_side

    def line_copy(step, from_line):
        target = lax.rem(part + step * PLANE, count)
        return hub_copy(1 + step, place * lines + from_line, 1, target, own_hubs_ref)

    def halo_copy(number, slot, offset, piece):
        landing_ref = early_ref if number < EARLY else extended_ref
        start = own_blocks + slot * slot_blocks + piece * piece_blocks
        blocks = pl.ds(start, piece_blocks)
        return pltpu.make_async_remote_copy(
            src_ref=packed_ref.at[number, pl.ds(piece * piece_blocks, piece_blocks)],
            dst_ref=landing_ref.at[blocks],
            send_sem=send_sems.at[number, piece], recv_sem=receive_sems.at[slot, piece],
            device_id=(lax.rem(part + offset + count, count), feat), device_id_type=MESH,
        )

    def present(number):
        target = part + ordered[number]
        return (target >= 0) & (target < count)

    def wait_sent(number, pieces):
        for piece in pieces:
            halo_copy(number, ordered_slots[number], ordered[number], piece).wait_send()

    early = range(PIECES - HELD)
    late = range(PIECES - HELD, PIECES)

    def gate(number, also=True):
        @pl.when(present(number) & also)
        def _():
            wait_sent(number, early)

    def pick(number):
        @pl.when(present(number))
        def _():
            for piece in range(PIECES):
                rows = pl.ds(piece * chunk, chunk)
                index = index_ref[rows, number : number + 1]
                packed_ref[number, pl.ds(piece * piece_blocks, piece_blocks)] = picked_rows(
                    index, table_ref, GROUPS
                ).reshape(piece_blocks, edge, width)
                if number < 2:
                    halo_copy(number, ordered_slots[number], ordered[number], piece).start()

    def send(number, also=True, pieces=range(PIECES)):
        @pl.when(present(number) & also)
        def _():
            for piece in pieces:
                halo_copy(number, ordered_slots[number], ordered[number], piece).start()

    inner = jnp.logical_not(outer)
    own_hubs = picked_rows(own_index, table_ref, GROUPS)
    own_hubs_ref[...] = own_hubs
    hub_home = (place * lines + line) * HUB_MOST
    hubs_ref[pl.ds(pl.multiple_of(hub_home, 16), HUB_MOST), :] = own_hubs
    for step in range(1, lines):
        line_copy(step, line).start()
    pick(0)
    pick(1)
    pick(2)
    pick(3)
    gate(0)
    send(2)
    send(3, inner)
    pick(4)
    pick(5)
    pick(6)
    pick(7)
    for step in range(1, lines):
        line_copy(step, lax.rem(line - step + lines, lines)).wait_recv()
    loads[3 + GROUPS].wait()
    loads[4 + GROUPS].wait()
    arrange_tiles(
        live_ref[0], rows_ref[...], cols_ref[...], own_blocks, slot_blocks,
        [arriving(offset) for offset in offsets],
        [arrives_early(offset) for offset in offsets], early_meta_ref, late_ref,
    )
    meta_copy = pltpu.make_async_copy(early_meta_ref, early_smem, load_sems.at[6 + GROUPS])
    meta_copy.start()
    late_copy = pltpu.make_async_copy(late_ref, late_smem, load_sems.at[7 + GROUPS])
    late_copy.start()
    gate(2)
    send(3, outer)
    send(4)
    hub_copy(0, place * lines, lines, across).start()
    send(5)
    gate(3)
    gate(4)
    send(6)
    send(7)
    hub_copy(0, across_place * lines, lines, across).wait_recv()
    pair_rows = 2 * lines * HUB_MOST
    pair_start = pair_place * lines * HUB_MOST
    owner_line = owner_col // PLANE
    owner_place = owner_col - owner_line * PLANE
    within = (owner_place * lines + owner_line) * HUB_MOST + rank_col - pair_start
    positions = lax.broadcasted_iota(jnp.int32, (hub_total, pair_rows), 1)
    chosen = (positions == within).astype(jnp.float32).astype(jnp.bfloat16)
    pair_hubs = hubs_ref[pl.ds(pl.multiple_of(pair_start, 16), pair_rows), :]
    near_hubs = jnp.dot(chosen, pair_hubs, preferred_element_type=jnp.float32)
    near_hubs_ref[...] = near_hubs.astype(jnp.bfloat16)
    hub_exchange = pltpu.make_async_remote_copy(
        src_ref=near_hubs_ref, dst_ref=far_hubs_ref,
        send_sem=hub_send_sems.at[1], recv_sem=hub_receive_sems.at[1],
        device_id=(far, feat), device_id_type=MESH,
    )
    hub_exchange.start()

    for slot, offset in enumerate(offsets):

        @pl.when(arrives_early(offset))
        def _():
            for piece in range(PIECES):
                halo_copy(0, slot, offset, piece).wait_recv()

    values_load.wait()
    meta_copy.wait()
    late_copy.wait()
    together = math.gcd(tile_slots, 12)

    def step(number, running):
        for inner in range(together):
            entry = number * together + inner
            product = jnp.dot(
                values_ref[early_smem[0, entry]], early_ref[early_smem[1, entry]],
                preferred_element_type=jnp.float32,
            )
            kept = jnp.broadcast_to(early_smem[2, entry], running.shape) > 0
            running = jnp.where(kept, running, 0.0) + product
            sums_ref[entry] = running
        return running

    lax.fori_loop(0, tile_slots // together, step, jnp.zeros((edge, width), jnp.float32))
    for block in range(vertex_rows // edge):
        summed = sums_ref[early_smem[3, block]]
        kept = jnp.broadcast_to(early_smem[4, block], summed.shape) > 0
        early_total_ref[block * edge : (block + 1) * edge, :] = jnp.where(kept, summed, 0.0)

    hub_exchange.wait_recv()
    hubs = near_hubs_ref[...].astype(jnp.float32) + far_hubs_ref[...].astype(jnp.float32)
    extended_ref[hub_block:] = hubs.astype(jnp.bfloat16).reshape(hub_total // edge, edge, width)
    for exchange in exchanges:
        exchange.wait_send()
    hub_copy(0, place * lines, lines, across).wait_send()
    hub_exchange.wait_send()
    for step in range(1, lines):
        line_copy(step, line).wait_send()
    for number in range(slots):
        gated = number in (0, 2, 3, 4)

        @pl.when(present(number))
        def _():
            wait_sent(number, late if gated else range(PIECES))

    for slot, offset in enumerate(offsets):

        @pl.when(arriving(offset) & jnp.logical_not(arrives_early(offset)))
        def _():
            for piece in range(PIECES):
                halo_copy(EARLY, slot, offset, piece).wait_recv()


def tiles_kernel(
    late_ref, values_ref, extended_ref, start_ref, bias_ref, out_ref, total_ref
):
    slots, edge, _ = values_ref.shape
    spare = out_ref.shape[0] // edge
    total_ref[: out_ref.shape[0], :] = start_ref[...]
    total_ref[out_ref.shape[0] :, :] = jnp.zeros((edge, out_ref.shape[1]), jnp.float32)
    live = late_ref[3, 0]
    together = math.gcd(slots, 12)

    def step(number, carry):
        products, places = [], []
        for inner in range(together):
            entry = number * together + inner
            places.append(jnp.where(entry < live, late_ref[1, entry], spare))
            products.append(
                jnp.dot(
                    values_ref[late_ref[0, entry]], extended_ref[late_ref[2, entry]],
                    preferred_element_type=jnp.float32,
                )
            )
        for place, product in zip(places, products):
            total_ref[pl.ds(pl.multiple_of(place * edge, edge), edge), :] += product
        return carry

    lax.fori_loop(0, (live + together - 1) // together, step, 0)
    summed = total_ref[: out_ref.shape[0], :] + bias_ref[...]
    out_ref[...] = jnp.maximum(summed, 0.0).astype(jnp.bfloat16)


def local(
    features, weight, out_bias, tile_values, tile_rows, tile_cols, tile_count, send_rows, hub_ids
):
    width = out_bias.shape[0]
    vertex_rows, depth = features.shape
    count = lax.axis_size("dom")
    _, slots, half_rows = send_rows.shape
    hub_total = hub_ids.shape[0]
    edge = tile_values.shape[1]
    vmem = pl.BlockSpec(memory_space=pltpu.VMEM)
    blocks = (vertex_rows + slots * half_rows + hub_total) // edge
    tile_slots = tile_values.shape[0]
    hbm = pl.BlockSpec(memory_space=pltpu.HBM)
    smem = pl.BlockSpec(memory_space=pltpu.SMEM)
    extended, values, early_total, late = pl.pallas_call(
        functools.partial(exchange_kernel, count),
        out_shape=[
            jax.ShapeDtypeStruct((blocks, edge, width), jnp.bfloat16),
            jax.ShapeDtypeStruct(tile_values.shape, jnp.bfloat16),
            jax.ShapeDtypeStruct((vertex_rows, width), jnp.float32),
            pltpu.SMEM((8, tile_slots), jnp.int32),
        ],
        in_specs=[hbm] * 7 + [smem],
        out_specs=[vmem] * 3 + [smem],
        scratch_shapes=[
            pltpu.VMEM((depth, vertex_rows), jnp.bfloat16),
            pltpu.VMEM(weight.shape, jnp.bfloat16),
            pltpu.VMEM((slots, half_rows), jnp.int32),
            pltpu.VMEM((1, hub_total), jnp.int32),
            pltpu.VMEM((1, tile_slots), jnp.int32),
            pltpu.VMEM((1, tile_slots), jnp.int32),
            pltpu.SemaphoreType.DMA((8 + GROUPS,)),
            pltpu.VMEM((blocks, edge, width), jnp.bfloat16),
            pltpu.VMEM((8, tile_slots), jnp.int32),
            pltpu.VMEM((8, tile_slots), jnp.int32),
            pltpu.SMEM((8, tile_slots), jnp.int32),
            pltpu.VMEM((tile_slots, edge, width), jnp.float32),
            pltpu.VMEM((width, vertex_rows), jnp.bfloat16),
            pltpu.VMEM((width, vertex_rows), jnp.bfloat16),
            pltpu.VMEM((width, vertex_rows), jnp.float32),
            pltpu.VMEM((vertex_rows // GROUPS, GROUPS * width), jnp.bfloat16),
            pltpu.VMEM((slots, half_rows), jnp.int32),
            pltpu.VMEM((half_rows, slots), jnp.int32),
            pltpu.VMEM((slots, half_rows // edge, edge, width), jnp.bfloat16),
            pltpu.VMEM((HUB_MOST, width), jnp.bfloat16),
            pltpu.VMEM((count * HUB_MOST, width), jnp.bfloat16),
            pltpu.VMEM((hub_total, width), jnp.bfloat16),
            pltpu.VMEM((hub_total, width), jnp.bfloat16),
            pltpu.SemaphoreType.DMA((2, GROUPS)),
            pltpu.SemaphoreType.DMA((slots, PIECES)),
            pltpu.SemaphoreType.DMA((slots, PIECES)),
            pltpu.SemaphoreType.DMA((count // PLANE + 1,)),
            pltpu.SemaphoreType.DMA((count // PLANE + 1,)),
        ],
        compiler_params=pltpu.CompilerParams(
            collective_id=0, has_side_effects=True, vmem_limit_bytes=32 << 20
        ),
    )(
        *[
            pltpu.with_memory_space_constraint(value, pltpu.HBM)
            for value in (
                jnp.transpose(features), weight, send_rows[0], hub_ids[None, :],
                tile_rows[None, :], tile_cols[None, :], tile_values,
            )
        ],
        tile_count,
    )
    return pl.pallas_call(
        tiles_kernel,
        out_shape=jax.ShapeDtypeStruct((vertex_rows, width), jnp.bfloat16),
        in_specs=[smem] + [vmem] * 4,
        out_specs=vmem,
        scratch_shapes=[
            pltpu.VMEM((vertex_rows + edge, width), jnp.float32),
        ],
        compiler_params=pltpu.CompilerParams(vmem_limit_bytes=24 << 20),
    )(late, values, extended, early_total, out_bias[None, :])


def solution(mesh):
    in_specs = (
        P("dom", "feat"),
        P(),
        P("feat"),
        P("dom", None, None),
        P("dom"),
        P("dom"),
        P("dom"),
        P("dom", None, None),
        P(),
    )
    out_specs = P("dom", "feat")

    def program(features, weight, out_bias, *rest):
        whole_lanes = out_bias.shape[0] % (LANES * mesh.shape["feat"]) == 0
        tile_values, send_rows, hub_ids = rest[0], rest[4], rest[5]
        edge = tile_values.shape[1]
        fits = mesh.shape["feat"] == 2 and mesh.shape["dom"] % PLANE == 0
        fits = fits and features.shape[0] % (mesh.shape["dom"] * GROUPS * edge) == 0
        fits = fits and send_rows.shape[2] % (PIECES * edge) == 0 and hub_ids.shape[0] % edge == 0
        body = local if fits and whole_lanes else local_any
        return jax.shard_map(
            body, mesh=mesh, in_specs=in_specs, out_specs=out_specs, check_vma=False
        )(features, weight, out_bias, *rest)

    return program
```
